32 devices in a mesh: groups: 2 (over y), tx: 4 (over z), ty: 2 (over x), ka: 2 (over core).
Axes of the slice: x: 2, y: 2, z: 4, core: 2. Of those that a mesh axis runs over, the one named last changes fastest.
Arguments:
- mask_raster: float32 [2048, 512], P(('groups', 'tx'), 'ty'), parts along dimension 0, may hold values from 0 to 1
- frag_rows: int32 [8, 2, 512], P(('groups', 'tx'), 'ty'), parts along dimension 0, may hold values from 8 to 215
- frag_cols: int32 [8, 2, 512], P(('groups', 'tx'), 'ty'), parts along dimension 0, may hold values from 8 to 215
- frag_length: int32 [8, 2, 512], P(('groups', 'tx'), 'ty'), parts along dimension 0, may hold values from 4 to 32
- frag_orient: int32 [8, 2, 512], P(('groups', 'tx'), 'ty'), parts along dimension 0, may hold values from 0 to 1
- frag_moves: int32 [8, 2, 2, 512], P(('groups', 'tx'), 'ty'), parts along dimension 0, may hold values from -4 to 4
- site_rows: int32 [8, 2, 2048], P(('groups', 'tx'), 'ty'), parts along dimension 0, may hold values from 1 to 254
- site_cols: int32 [8, 2, 2048], P(('groups', 'tx'), 'ty'), parts along dimension 0, may hold values from 1 to 254
- spectra: float32 [16, 2, 128, 128], P('ka'), may hold values from -24 to 24
- weights: float32 [16], P('ka'), may hold values from 0.05 to 1
- tolerance: int32 [2], replicated, may hold values from 1 to 16
Outputs:
- intensity: float32 [2048, 512], P(('groups', 'tx'), 'ty'), parts along dimension 0
- corrected_mask: float32 [2048, 512], P(('groups', 'tx'), 'ty'), parts along dimension 0
- edge_errors: float32 [8, 2, 2, 2048], P(('groups', 'tx'), 'ty'), parts along dimension 0
- peak_error: float32 [4], P('groups'), parts along dimension 0
- converged_share: float32 [4], P('groups'), parts along dimension 0
The draws below stay inside these ranges and needn't reach their ends.
There are 2 independent parts, one for each index of `groups`. The reference program is written for one: setup_inputs(seed, part) draws one part's arguments, and reference() takes and returns one part's arrays. A program takes and returns all parts, laid end to end along the dimension named above; an argument that names none is the same for every part. Nothing has to cross between parts.
All inputs are finite; a program needn't handle non-finite values.
Results may differ from the reference program's by a relative error of at most 0.0003.
Values sent between devices are 32-bit elements; how exact they have to be, the bound alone decides.
A program may use at most 64 MiB of HBM per device.

```python
import math
import jax
import jax.numpy as jnp
from jax import lax

TILE = 256
HALO = 128
BAND = 128
KERNELS = 16
NFRAG = 512
SITES = 2048
ITERS = 2
ROWS = 1024
COLS = 512
N_TX = 4
N_TY = 2


def draw_spectra(key, part):
    shape = (KERNELS, 2, BAND, BAND)
    scale = (TILE + 2 * HALO) / BAND
    values = jnp.clip(jax.random.normal(key, shape, jnp.float32), -6.0, 6.0)
    first = jnp.arange(BAND)[:, None] == BAND // 2
    second = jnp.arange(BAND)[None, :] == BAND // 2
    factor = jnp.where(first & second, 0.02, 1.0)
    return (values * scale * factor[None, None]).astype(jnp.float32)


def plant(drawn, key, low, top_value):
    spot = [jax.random.randint(jax.random.fold_in(key, axis), (), 0, length) for axis, length in enumerate(drawn.shape)]
    main_axis = drawn.shape.index(max(drawn.shape))
    neighbour = spot[:main_axis] + [(spot[main_axis] + 1) % drawn.shape[main_axis]] + spot[main_axis + 1:]
    return drawn.at[tuple(spot)].set(low).at[tuple(neighbour)].set(top_value)


def steps_of(stream_key, dims, pieces, low, largest):
    loudness = 1.0
    for dim, shards_of in pieces:
        heights = jax.random.uniform(jax.random.fold_in(jax.random.fold_in(stream_key, 6), dim), (shards_of,), jnp.float32, low / len(pieces), largest / len(pieces))
        loudness = loudness * jnp.repeat(jnp.exp(heights), dims[dim] // shards_of).reshape((-1,) + (1,) * (len(dims) - 1 - dim))
    return loudness


def setup_inputs(seed: int = 0, part: int = 0) -> dict:
    key_list = jax.random.split(jax.random.key(seed), 12)
    part_keys = jax.random.split(jax.random.fold_in(key_list[11], part), 12)
    mask_raster = jnp.clip(1.0 * jax.random.uniform(part_keys[0], (ROWS, COLS), jnp.float32) ** steps_of(part_keys[0], (ROWS, COLS), ((0, 4), (1, 2)), -0.2, 0.2), 0.0, 1.0)
    frag_rows = plant(jax.random.randint(part_keys[1], (N_TX, N_TY, NFRAG), 8, TILE - 40), jax.random.fold_in(part_keys[1], 1), 8, (TILE - 40) - 1).astype(jnp.int32)
    frag_cols = plant(jax.random.randint(part_keys[2], (N_TX, N_TY, NFRAG), 8, TILE - 40), jax.random.fold_in(part_keys[2], 1), 8, (TILE - 40) - 1).astype(jnp.int32)
    frag_length = plant(jax.random.randint(part_keys[3], (N_TX, N_TY, NFRAG), 4, 33), jax.random.fold_in(part_keys[3], 1), 4, 32).astype(jnp.int32)
    frag_orient = plant(jax.random.randint(part_keys[4], (N_TX, N_TY, NFRAG), 0, 2), jax.random.fold_in(part_keys[4], 1), 0, 1).astype(jnp.int32)
    frag_moves = plant(jax.random.randint(part_keys[5], (N_TX, N_TY, ITERS, NFRAG), -4, 5), jax.random.fold_in(part_keys[5], 1), -4, 4).astype(jnp.int32)
    site_rows = plant(jax.random.randint(part_keys[6], (N_TX, N_TY, SITES), 1, TILE - 1), jax.random.fold_in(part_keys[6], 1), 1, (TILE - 1) - 1).astype(jnp.int32)
    site_cols = plant(jax.random.randint(part_keys[7], (N_TX, N_TY, SITES), 1, TILE - 1), jax.random.fold_in(part_keys[7], 1), 1, (TILE - 1) - 1).astype(jnp.int32)
    spectra = draw_spectra(jax.random.fold_in(key_list[11], 71), part)
    weights = jnp.clip(jnp.exp(math.log(1.0) - 2.9957323 * jax.random.uniform(key_list[9], (KERNELS,), jnp.float32) ** steps_of(key_list[9], (KERNELS,), ((0, 2),), -0.2, 0.2)), 0.05, 1.0)
    tolerance = jax.random.randint(key_list[10], (ITERS,), 1, 17).astype(jnp.int32)
    return {"mask_raster": mask_raster, "frag_rows": frag_rows, "frag_cols": frag_cols, "frag_length": frag_length, "frag_orient": frag_orient, "frag_moves": frag_moves, "site_rows": site_rows, "site_cols": site_cols, "spectra": spectra, "weights": weights, "tolerance": tolerance}


LEVEL = 0.4
SLOPE_FLOOR = 0.05
SHARPNESS = 8.0

def strip_sum(row_start, col_start, frag_len, orient, shift, extent):
    lower = jnp.minimum(shift, 0)
    upper = jnp.maximum(shift, 0)
    along_rows = orient == 0
    row_low = jnp.where(along_rows, row_start, row_start + lower)
    row_high = jnp.where(along_rows, row_start + frag_len, row_start + upper)
    col_low = jnp.where(along_rows, col_start + lower, col_start)
    col_high = jnp.where(along_rows, col_start + upper, col_start + frag_len)
    position = jnp.arange(extent, dtype=jnp.int32)
    signs = jnp.sign(shift).astype(jnp.float32)
    row_select = ((position[:, None] >= row_low[None, :]) & (position[:, None] < row_high[None, :])).astype(jnp.float32) * signs[None, :]
    col_select = ((position[None, :] >= col_low[:, None]) & (position[None, :] < col_high[:, None])).astype(jnp.float32)
    return jnp.dot(row_select.astype(jnp.bfloat16), col_select.astype(jnp.bfloat16), preferred_element_type=jnp.float32)

def edge_error(image, rows_at, cols_at):
    flat = image.reshape(-1)
    width = image.shape[1]

    def sample(delta_row, delta_col):
        return flat[(rows_at + delta_row) * width + cols_at + delta_col]
    center = sample(0, 0)
    grad_rows = (sample(1, 0) - sample(-1, 0)) * 0.5
    grad_cols = (sample(0, 1) - sample(0, -1)) * 0.5
    slope = jnp.sqrt(grad_rows * grad_rows + grad_cols * grad_cols)
    return (center - LEVEL) / jnp.maximum(slope, SLOPE_FLOOR)

def reference(mask_raster, frag_rows, frag_cols, frag_length, frag_orient, frag_moves, site_rows, site_cols, spectra, weights, tolerance):
    tiles_x = mask_raster.shape[0] // TILE
    tiles_y = mask_raster.shape[1] // TILE
    count = tiles_x * tiles_y
    ext_size = TILE + 2 * HALO
    freq = (jnp.arange(BAND, dtype=jnp.int32) - BAND // 2) % ext_size
    kernel_spec = spectra[:, 0] + 1j * spectra[:, 1]
    current = mask_raster
    flat_rows = frag_rows.reshape(count, NFRAG)
    flat_cols = frag_cols.reshape(count, NFRAG)
    flat_len = frag_length.reshape(count, NFRAG)
    flat_orient = frag_orient.reshape(count, NFRAG)
    errors_all = []
    peaks = []
    shares = []
    images = None
    for iteration in range(ITERS):
        flat_moves = frag_moves[:, :, iteration, :].reshape(count, NFRAG)
        strips = lax.map(lambda items: strip_sum(items[0], items[1], items[2], items[3], items[4], TILE), (flat_rows, flat_cols, flat_len, flat_orient, flat_moves))
        region = strips.reshape(tiles_x, tiles_y, TILE, TILE).transpose(0, 2, 1, 3).reshape(tiles_x * TILE, tiles_y * TILE)
        current = jnp.clip(current + region, 0.0, 1.0)
        padded = jnp.pad(current, HALO)

        def image_tile(number):
            first = (number // tiles_y * TILE).astype(jnp.int32)
            second = (number % tiles_y * TILE).astype(jnp.int32)
            window = lax.dynamic_slice(padded, (first, second), (ext_size, ext_size))
            spectrum = jnp.fft.fft2(window)
            kept = spectrum[freq][:, freq]
            product = kernel_spec * kept[None]
            full = jnp.zeros((product.shape[0], ext_size, ext_size), product.dtype)
            full = full.at[:, freq[:, None], freq[None, :]].set(product)
            field = jnp.fft.ifft2(full, axes=(1, 2))[:, HALO:HALO + TILE, HALO:HALO + TILE]
            return lax.optimization_barrier(jnp.sum(weights[:, None, None] * (field.real * field.real + field.imag * field.imag), axis=0))
        images = lax.map(image_tile, jnp.arange(count, dtype=jnp.int32))
        errors_now = jax.vmap(edge_error)(images, site_rows.reshape(count, SITES), site_cols.reshape(count, SITES))
        errors_all.append(errors_now.reshape(tiles_x, tiles_y, SITES))
        peaks.append(jnp.max(jnp.abs(errors_now)))
        limit = tolerance[iteration].astype(jnp.float32) / 8.0
        shares.append(jnp.mean(jax.nn.sigmoid(SHARPNESS * (limit - jnp.abs(errors_now)))))
    intensity = images.reshape(tiles_x, tiles_y, TILE, TILE).transpose(0, 2, 1, 3).reshape(tiles_x * TILE, tiles_y * TILE)
    edge_errors = jnp.stack(errors_all, axis=2)
    return (intensity, current, edge_errors, jnp.stack(peaks), jnp.stack(shares))
```

```python
import functools
import math

import jax
import jax.numpy as jnp
import ml_dtypes
import numpy as np
from jax import lax
from jax.experimental import pallas as pl
from jax.experimental.pallas import tpu as pltpu
from jax.sharding import PartitionSpec as P

HALO = 128
BAND = 128
ITERS = 2

LEVEL = 0.4
SLOPE_FLOOR = 0.05
SHARPNESS = 8.0
CHUNK = 256
OPERANDS = 18
VMEM_LIMIT = 32 * 1024 * 1024
MESH = pl.DeviceIdType.MESH
F32 = jnp.float32
BF16 = jnp.bfloat16


def pieces_of(table):
    high = table.astype(ml_dtypes.bfloat16)
    rest = table - high.astype(np.float64)
    middle = rest.astype(ml_dtypes.bfloat16)
    low = (rest - middle.astype(np.float64)).astype(ml_dtypes.bfloat16)
    return high, middle, low


def tables(tile):
    ext = tile + 2 * HALO
    half = BAND // 2
    step = 2.0 * math.pi / ext
    rows = -(-(2 * half + 1) // 16) * 16
    span = np.arange(ext) - (ext - 1) / 2
    positive = np.arange(half + 1)
    freq = np.arange(BAND) - half
    forward = np.zeros((rows, ext))
    forward[: half + 1] = np.cos(step * positive[:, None] * span[None])
    forward[half + 1 : 2 * half + 1] = np.sin(step * positive[1:, None] * span[None])
    phase = step * span[:, None] * freq[None]
    across = np.concatenate([np.cos(phase), np.sin(phase)], axis=1)
    expand = np.zeros((2 * BAND, 2 * BAND))
    for place, number in enumerate(freq):
        expand[place, abs(number)] = 1.0
        if number != 0:
            expand[BAND + place, half + abs(number)] = np.sign(number)
    angle = step * (np.arange(tile // 2)[:, None] + 0.5) * freq[None]
    back_rows = np.concatenate([np.cos(angle), np.sin(angle)], axis=0) / ext
    back_cols = np.concatenate([np.cos(angle.T), np.sin(angle.T)], axis=1) / ext
    flip = np.eye(tile // 2)[::-1].astype(ml_dtypes.bfloat16)
    high, middle, low = pieces_of(back_rows)
    rows6 = np.concatenate([high, high, middle, high, middle, low], axis=1)
    high, middle, low = pieces_of(back_cols)
    cols6 = np.concatenate([high, high, middle, high, middle, low], axis=0)
    return (
        np.concatenate(pieces_of(forward), axis=0),
        np.concatenate(pieces_of(across), axis=0),
        np.concatenate([expand] * 3, axis=1).astype(ml_dtypes.bfloat16),
        rows6,
        cols6,
        np.concatenate([flip] * 3, axis=1),
        np.concatenate([flip] * 3, axis=0),
    )


def split(value):
    high = value.astype(BF16)
    low = (value - high.astype(F32)).astype(BF16)
    return high, low


def split3(value):
    high = value.astype(BF16)
    rest = value - high.astype(F32)
    middle = rest.astype(BF16)
    low = (rest - middle.astype(F32)).astype(BF16)
    return high, middle, low


def dot(left, right):
    return jnp.dot(left, right, preferred_element_type=F32)


def strip_sum(row_start, col_start, frag_len, orient, shift, extent):
    lower = jnp.minimum(shift, 0)
    upper = jnp.maximum(shift, 0)
    along = orient == 0
    row_low = jnp.where(along, row_start, row_start + lower)
    row_high = jnp.where(along, row_start + frag_len, row_start + upper)
    col_low = jnp.where(along, col_start + lower, col_start)
    col_high = jnp.where(along, col_start + upper, col_start + frag_len)
    position = lax.broadcasted_iota(jnp.int32, (extent, shift.shape[1]), 0)
    signs = jnp.where(shift > 0, 1.0, jnp.where(shift < 0, -1.0, 0.0))
    row_select = jnp.where((position >= row_low) & (position < row_high), signs, 0.0).astype(BF16)
    col_select = jnp.where((position >= col_low) & (position < col_high), 1.0, 0.0).astype(BF16)
    return lax.dot_general(
        row_select, col_select, (((1,), (1,)), ((), ())), preferred_element_type=F32
    )


def kernel(sizes, *refs):
    away, outs = refs[:OPERANDS], refs[OPERANDS : OPERANDS + 4]
    here, rest = refs[OPERANDS + 4 : 2 * OPERANDS + 4], refs[2 * OPERANDS + 4 :]
    sems = rest[-1]
    copies = [
        pltpu.make_async_copy(src, dst, sems.at[i]) for i, (src, dst) in enumerate(zip(away, here))
    ]

    def need(*numbers):
        for number in numbers:
            copies[number].wait()

    def start(*numbers):
        for number in numbers:
            copies[number].start()

    body(sizes, start, need, away[8], *here, *outs, *rest[:-1])


def body(
    sizes,
    begin,
    need,
    spec_away,
    mask_ref,
    frow_ref,
    fcol_ref,
    flen_ref,
    fori_ref,
    fmove_ref,
    srow_ref,
    scol_ref,
    spec_ref,
    weight_ref,
    tol_ref,
    forward_ref,
    across_ref,
    expand_ref,
    rows_ref,
    cols_ref,
    flip_wide_ref,
    flip_tall_ref,
    intensity_ref,
    mask_out_ref,
    errors_ref,
    stats_ref,
    ext,
    hext,
    spec_rx,
    wv,
    wv_rx,
    sbuf,
    folded,
    choose,
    img,
    img_rx,
    err,
    err_rx,
    stat,
    stat_rx,
    halo_send,
    halo_recv,
    ka_send,
    ka_recv,
    stat_send,
    stat_recv,
):
    n_tx, n_ty, n_ka = sizes
    count = n_tx * n_ty * n_ka
    tile = mask_ref.shape[0]
    wide = ext.shape[0]
    sites = srow_ref.shape[2]
    kernels = spec_ref.shape[0]
    group = lax.axis_index("groups")
    tx = lax.axis_index("tx")
    ty = lax.axis_index("ty")
    ka = lax.axis_index("ka")
    me = (tx * n_ty + ty) * n_ka + ka

    def place(number):
        return (
            group,
            lax.div(number, n_ty * n_ka),
            lax.rem(lax.div(number, n_ka), n_ty),
            lax.rem(number, n_ka),
        )

    def remote(src, dst, send, recv, target):
        return pltpu.make_async_remote_copy(
            src_ref=src, dst_ref=dst, send_sem=send, recv_sem=recv, device_id=target, device_id_type=MESH
        )

    begin(1, 2, 3, 4, 5, 0, 9, 11, 12, 8, 13, 14, 15, 16, 17, 6, 7, 10)
    barrier = pltpu.get_barrier_semaphore()

    def greet(offset, carry):
        pl.semaphore_signal(
            barrier, inc=1, device_id=place(lax.rem(me + offset, count)), device_id_type=MESH
        )
        return carry

    lax.fori_loop(1, count, greet, 0)

    need(1, 2, 3, 4, 5, 0)
    fragments = (frow_ref[0], fcol_ref[0], flen_ref[0], fori_ref[0])
    first = jnp.clip(mask_ref[...] + strip_sum(*fragments, fmove_ref[0, 0, 0:1, :], tile), 0.0, 1.0)
    second = jnp.clip(first + strip_sum(*fragments, fmove_ref[0, 0, 1:2, :], tile), 0.0, 1.0)
    mask_out_ref[...] = second
    ext[HALO : HALO + tile, :] = jnp.where(ka == 0, first, second)
    need(9)
    for k in range(kernels):
        wv[k : k + 1, :] = jnp.full((1, 128), weight_ref[k], F32)

    pl.semaphore_wait(barrier, count - 1)

    partner = (group, tx, ty, 1 - ka)
    up = (group, tx - 1, ty, ka)
    down = (group, tx + 1, ty, ka)
    left = (group, tx, ty - 1, ka)
    right = (group, tx, ty + 1, ka)
    to_up = remote(
        ext.at[pl.ds(HALO, HALO)], ext.at[pl.ds(HALO + tile, HALO)], halo_send.at[0], halo_recv.at[0], up
    )
    to_down = remote(
        ext.at[pl.ds(tile, HALO)], ext.at[pl.ds(0, HALO)], halo_send.at[1], halo_recv.at[1], down
    )

    @pl.when(tx > 0)
    def _():
        to_up.start()

    @pl.when(tx < n_tx - 1)
    def _():
        to_down.start()

    to_spec = remote(spec_away, spec_rx, ka_send.at[0], ka_recv.at[0], partner)
    to_wv = remote(wv, wv_rx, ka_send.at[1], ka_recv.at[1], partner)
    to_spec.start()
    to_wv.start()

    need(7)
    position = lax.broadcasted_iota(jnp.int32, (tile, CHUNK), 0)
    for start in range(0, sites, CHUNK):
        at_cols = scol_ref[0, :, start : start + CHUNK]
        choose[:, start : start + CHUNK] = jnp.where(position == at_cols, 1.0, 0.0).astype(BF16)

    @pl.when(tx == 0)
    def _():
        ext[0:HALO, :] = jnp.zeros((HALO, tile), F32)

    @pl.when(tx == n_tx - 1)
    def _():
        ext[HALO + tile : wide, :] = jnp.zeros((HALO, tile), F32)

    @pl.when(ty == 0)
    def _():
        hext[0] = jnp.zeros(hext.shape[1:], F32)

    @pl.when(ty == n_ty - 1)
    def _():
        hext[3] = jnp.zeros(hext.shape[1:], F32)

    @pl.when(tx > 0)
    def _():
        to_down.wait_recv()

    @pl.when(tx < n_tx - 1)
    def _():
        to_up.wait_recv()

    rows = hext.shape[1]
    need(11)
    high, middle, low = split3(ext[...])
    by_high = dot(forward_ref[...], high)
    by_middle = dot(forward_ref[0 : 2 * rows, :], middle)
    by_low = dot(forward_ref[0:rows, :], low)
    half = (by_low + by_high[2 * rows :] + by_middle[rows:]) + (by_high[rows : 2 * rows] + by_middle[:rows])
    half = half + by_high[:rows]
    hext[1] = half[:, :HALO]
    hext[2] = half[:, HALO:]
    to_left = remote(hext.at[1], hext.at[3], halo_send.at[2], halo_recv.at[2], left)
    to_right = remote(hext.at[2], hext.at[0], halo_send.at[3], halo_recv.at[3], right)

    @pl.when(ty > 0)
    def _():
        to_left.start()

    @pl.when(ty < n_ty - 1)
    def _():
        to_right.start()

    @pl.when(ty > 0)
    def _():
        to_right.wait_recv()

    @pl.when(ty < n_ty - 1)
    def _():
        to_left.wait_recv()

    need(12, 13)
    whole = jnp.concatenate([hext[0], hext[1], hext[2], hext[3]], axis=1)
    high, middle, low = split3(whole)
    by_high = dot(jnp.concatenate([high, middle, low], axis=0), across_ref[0:wide, :])
    by_middle = dot(jnp.concatenate([high, middle], axis=0), across_ref[wide : 2 * wide, :])
    by_low = dot(high, across_ref[2 * wide :, :])
    full = (by_low + by_high[2 * rows :] + by_middle[rows:]) + (by_high[rows : 2 * rows] + by_middle[:rows])
    full = full + by_high[:rows]
    full = jnp.concatenate([full, jnp.zeros((2 * BAND - rows, 2 * BAND), F32)], axis=0)
    mixed = dot(expand_ref[...], jnp.concatenate(split3(full), axis=0))
    sbuf[0] = mixed[:BAND, :BAND] - mixed[BAND:, BAND:]
    sbuf[1] = -(mixed[BAND:, :BAND] + mixed[:BAND, BAND:])

    mid = tile // 2
    folded[...] = jnp.zeros_like(folded)

    def kernel_image(spectra, scales, k):
        scale = jnp.sqrt(scales[pl.ds(k, 1), :])
        k_re = spectra[k, 0] * scale
        k_im = spectra[k, 1] * scale
        s_re = sbuf[0]
        s_im = sbuf[1]
        p_re = k_re * s_re - k_im * s_im
        p_im = k_re * s_im + k_im * s_re
        high, middle, low = split3(jnp.concatenate([p_re, p_im], axis=1))
        parts = dot(
            rows_ref[...], jnp.concatenate([high, middle, high, low, middle, high], axis=0)
        )
        even_re, even_im = parts[:mid, :BAND], parts[:mid, BAND:]
        odd_re, odd_im = parts[mid:, :BAND], parts[mid:, BAND:]
        inner = jnp.concatenate(
            [even_re - odd_im, even_re + odd_im, even_im + odd_re, even_im - odd_re], axis=0
        )
        high, middle, low = split3(inner)
        turned = dot(
            jnp.concatenate([high, middle, high, low, middle, high], axis=1), cols_ref[...]
        )
        re_cos, re_sin = turned[:tile, :mid], turned[:tile, mid:]
        im_cos, im_sin = turned[tile:, :mid], turned[tile:, mid:]
        f_re, f_im = re_cos - im_sin, im_cos + re_sin
        near = f_re * f_re + f_im * f_im
        f_re, f_im = re_cos + im_sin, im_cos - re_sin
        return near, f_re * f_re + f_im * f_im

    def add_pair(spectra, scales, k):
        near_a, far_a = kernel_image(spectra, scales, 4 * k)
        near_b, far_b = kernel_image(spectra, scales, 4 * k + 1)
        near_c, far_c = kernel_image(spectra, scales, 4 * k + 2)
        near_d, far_d = kernel_image(spectra, scales, 4 * k + 3)
        folded[:, :mid] += (near_a + near_b) + (near_c + near_d)
        folded[:, mid:] += (far_a + far_b) + (far_c + far_d)

    def add_one(spectra, scales, k):
        near, far = kernel_image(spectra, scales, k)
        folded[:, :mid] += near
        folded[:, mid:] += far

    def own_step(k, carry):
        add_pair(spec_ref, wv, k)
        return carry

    def rx_step(k, carry):
        add_pair(spec_rx, wv_rx, k)
        return carry

    need(8, 14, 15)
    lax.fori_loop(0, kernels // 4, own_step, 0)
    for k in range(kernels // 4 * 4, kernels):
        add_one(spec_ref, wv, k)
    to_spec.wait_recv()
    to_wv.wait_recv()
    lax.fori_loop(0, kernels // 4, rx_step, 0)
    for k in range(kernels // 4 * 4, kernels):
        add_one(spec_rx, wv_rx, k)

    need(16, 17)
    lower = jnp.concatenate(split3(folded[mid:, :]), axis=0)
    ordered = jnp.concatenate([dot(flip_wide_ref[...], lower), folded[:mid, :]], axis=0)
    lower = jnp.concatenate(split3(ordered[:, mid:]), axis=1)
    img[...] = jnp.concatenate([dot(lower, flip_tall_ref[...]), ordered[:, :mid]], axis=1)
    to_img = remote(img, img_rx, ka_send.at[2], ka_recv.at[2], partner)
    to_img.start()

    image = img[...]
    grad_rows = (pltpu.roll(image, tile - 1, 0) - pltpu.roll(image, 1, 0)) * 0.5
    grad_cols = (pltpu.roll(image, tile - 1, 1) - pltpu.roll(image, 1, 1)) * 0.5
    slope = jnp.sqrt(grad_rows * grad_rows + grad_cols * grad_cols)
    error_map = (image - LEVEL) / jnp.maximum(slope, SLOPE_FLOOR)
    high, low = split(error_map)
    need(6, 10)
    limit = tol_ref[ka].astype(F32) / 8.0
    peak = jnp.zeros((1, CHUNK), F32)
    total = jnp.zeros((1, CHUNK), F32)
    for start in range(0, sites, CHUNK):
        at_rows = srow_ref[0, :, start : start + CHUNK]
        picked = dot(high, choose[:, start : start + CHUNK]) + dot(low, choose[:, start : start + CHUNK])
        errors = jnp.sum(jnp.where(position == at_rows, picked, 0.0), axis=0, keepdims=True)
        err[:, start : start + CHUNK] = errors
        size = jnp.abs(errors)
        peak = jnp.maximum(peak, size)
        total = total + 1.0 / (1.0 + jnp.exp(-SHARPNESS * (limit - size)))
    stat[0:1, :] = functools.reduce(
        jnp.maximum, [peak[:, i : i + 128] for i in range(0, CHUNK, 128)]
    )
    stat[1:2, :] = functools.reduce(
        jnp.add, [total[:, i : i + 128] for i in range(0, CHUNK, 128)]
    )
    to_err = remote(err, err_rx, ka_send.at[3], ka_recv.at[3], partner)
    to_err.start()

    def to_stat(offset):
        return remote(
            stat,
            stat_rx.at[me],
            stat_send.at[offset],
            stat_recv.at[me],
            place(lax.rem(me + offset, count)),
        )

    def send_stat(offset, carry):
        to_stat(offset).start()
        return carry

    lax.fori_loop(1, count, send_stat, 0)
    stat_rx[pl.ds(me, 1)] = stat[...][None]

    to_img.wait_recv()
    intensity_ref[...] = jnp.where(ka == ITERS - 1, image, img_rx[...])
    to_err.wait_recv()
    mine = err[...]
    theirs = err_rx[...]
    errors_ref[0, 0, 0:1, :] = jnp.where(ka == 0, mine, theirs)
    errors_ref[0, 0, 1:2, :] = jnp.where(ka == 0, theirs, mine)

    def wait_stat(offset, carry):
        to_stat(offset).wait_send()
        source = lax.rem(me + offset, count)
        remote(
            stat, stat_rx.at[source], stat_send.at[offset], stat_recv.at[source], place(source)
        ).wait_recv()
        return carry

    lax.fori_loop(1, count, wait_stat, 0)

    for which in range(ITERS):
        rows_of = range(which, count, n_ka)
        stats_ref[which : which + 1, :] = functools.reduce(
            jnp.maximum, [stat_rx[number, 0:1, :] for number in rows_of]
        )
        stats_ref[ITERS + which : ITERS + which + 1, :] = functools.reduce(
            jnp.add, [stat_rx[number, 1:2, :] for number in rows_of]
        )

    @pl.when(tx > 0)
    def _():
        to_up.wait_send()

    @pl.when(tx < n_tx - 1)
    def _():
        to_down.wait_send()

    @pl.when(ty > 0)
    def _():
        to_left.wait_send()

    @pl.when(ty < n_ty - 1)
    def _():
        to_right.wait_send()

    for copy in (to_spec, to_wv, to_img, to_err):
        copy.wait_send()


def write(scale, image, mask, errors, stats, image_out, mask_out, errors_out, peaks, shares, sems):
    copies = [
        pltpu.make_async_copy(src, dst, sems.at[i])
        for i, (src, dst) in enumerate(((image, image_out), (mask, mask_out), (errors, errors_out)))
    ]
    for copy in copies:
        copy.start()
    for i in range(ITERS):
        peaks[i] = jnp.max(stats[i : i + 1, :])
        shares[i] = jnp.sum(stats[ITERS + i : ITERS + i + 1, :]) * scale
    for copy in copies:
        copy.wait()


def shards(sizes, *args):
    mask_raster, spectra = args[0], args[8]
    site_count = args[6].shape[2]
    tile = mask_raster.shape[0]
    wide = tile + 2 * HALO
    consts = [jnp.asarray(a) for a in tables(tile)]
    rows = consts[0].shape[0] // 3
    kernels = spectra.shape[0]
    count = sizes[0] * sizes[1] * sizes[2]
    vmem = pl.BlockSpec(memory_space=pltpu.VMEM)
    smem = pl.BlockSpec(memory_space=pltpu.SMEM)
    dma = pltpu.SemaphoreType.DMA
    operands = tuple(
        pltpu.with_memory_space_constraint(a, pltpu.HBM) for a in (*args, *consts)
    )
    local = [
        (pltpu.SMEM if number in (9, 10) else pltpu.VMEM)(a.shape, a.dtype)
        for number, a in enumerate(operands)
    ]
    tile_shape = (tile, tile)
    error_shape = (1, 1, ITERS, site_count)
    results = pl.pallas_call(
            functools.partial(kernel, sizes),
            out_shape=(
                pltpu.VMEM(tile_shape, F32),
                pltpu.VMEM(tile_shape, F32),
                pltpu.VMEM(error_shape, F32),
                pltpu.VMEM((8, 128), F32),
            ),
            in_specs=[pl.BlockSpec(memory_space=pltpu.HBM)] * OPERANDS,
            out_specs=(vmem,) * 4,
            scratch_shapes=local
            + [
                pltpu.VMEM((wide, tile), F32),
                pltpu.VMEM((4, rows, HALO), F32),
                pltpu.VMEM(spectra.shape, F32),
                pltpu.VMEM((kernels, 128), F32),
                pltpu.VMEM((kernels, 128), F32),
                pltpu.VMEM((2, BAND, BAND), F32),
                pltpu.VMEM((tile, tile), F32),
                pltpu.VMEM((tile, site_count), BF16),
                pltpu.VMEM((tile, tile), F32),
                pltpu.VMEM((tile, tile), F32),
                pltpu.VMEM((1, site_count), F32),
                pltpu.VMEM((1, site_count), F32),
                pltpu.VMEM((2, 128), F32),
                pltpu.VMEM((count, 2, 128), F32),
                dma((4,)),
                dma((4,)),
                dma((4,)),
                dma((4,)),
                dma((count,)),
                dma((count,)),
                dma((OPERANDS,)),
            ],
            compiler_params=pltpu.CompilerParams(
                collective_id=0, has_side_effects=True, vmem_limit_bytes=VMEM_LIMIT
            ),
        )(*operands)
    hbm = pl.BlockSpec(memory_space=pltpu.HBM)
    return tuple(
        pl.pallas_call(
            functools.partial(write, 1.0 / (site_count * sizes[0] * sizes[1])),
            out_shape=(
                jax.ShapeDtypeStruct(tile_shape, F32),
                jax.ShapeDtypeStruct(tile_shape, F32),
                jax.ShapeDtypeStruct(error_shape, F32),
                jax.ShapeDtypeStruct((ITERS,), F32),
                jax.ShapeDtypeStruct((ITERS,), F32),
            ),
            in_specs=[vmem] * 4,
            out_specs=(hbm, hbm, hbm, smem, smem),
            scratch_shapes=[dma((3,))],
            compiler_params=pltpu.CompilerParams(vmem_limit_bytes=VMEM_LIMIT),
        )(*results)
    )


def solution(mesh):
    sizes = tuple(mesh.shape[axis] for axis in ("tx", "ty", "ka"))
    assert sizes[2] == ITERS
    placed = (
        P(("groups", "tx"), "ty"),
        P(("groups", "tx"), "ty", None),
        P(("groups", "tx"), "ty", None),
        P(("groups", "tx"), "ty", None),
        P(("groups", "tx"), "ty", None),
        P(("groups", "tx"), "ty", None, None),
        P(("groups", "tx"), "ty", None),
        P(("groups", "tx"), "ty", None),
        P("ka", None, None, None),
        P("ka"),
        P(),
    )
    return jax.shard_map(
        functools.partial(shards, sizes),
        mesh=mesh,
        in_specs=placed,
        out_specs=(
            P(("groups", "tx"), "ty"),
            P(("groups", "tx"), "ty"),
            P(("groups", "tx"), "ty", None, None),
            P("groups"),
            P("groups"),
        ),
        check_vma=False,
    )
```

```python
import functools
import math

import jax
import jax.numpy as jnp
import ml_dtypes
import numpy as np
from jax import lax
from jax.experimental import pallas as pl
from jax.experimental.pallas import tpu as pltpu
from jax.sharding import PartitionSpec as P

HALO = 128
BAND = 128
ITERS = 2

LEVEL = 0.4
SLOPE_FLOOR = 0.05
SHARPNESS = 8.0
CHUNK = 256
OPERANDS = 18
VMEM_LIMIT = 32 * 1024 * 1024
MESH = pl.DeviceIdType.MESH
F32 = jnp.float32
BF16 = jnp.bfloat16


def pieces_of(table):
    high = table.astype(ml_dtypes.bfloat16)
    rest = table - high.astype(np.float64)
    middle = rest.astype(ml_dtypes.bfloat16)
    low = (rest - middle.astype(np.float64)).astype(ml_dtypes.bfloat16)
    return high, middle, low


def tables(tile):
    ext = tile + 2 * HALO
    half = BAND // 2
    step = 2.0 * math.pi / ext
    rows = -(-(2 * half + 1) // 16) * 16
    span = np.arange(ext) - (ext - 1) / 2
    positive = np.arange(half + 1)
    freq = np.arange(BAND) - half
    forward = np.zeros((rows, ext))
    forward[: half + 1] = np.cos(step * positive[:, None] * span[None])
    forward[half + 1 : 2 * half + 1] = np.sin(step * positive[1:, None] * span[None])
    phase = step * span[:, None] * freq[None]
    across = np.concatenate([np.cos(phase), np.sin(phase)], axis=1)
    expand = np.zeros((2 * BAND, 2 * BAND))
    for place, number in enumerate(freq):
        expand[place, abs(number)] = 1.0
        if number != 0:
            expand[BAND + place, half + abs(number)] = np.sign(number)
    angle = step * (np.arange(tile // 2)[:, None] + 0.5) * freq[None]
    back_rows = np.concatenate([np.cos(angle), np.sin(angle)], axis=0) / ext
    back_cols = np.concatenate([np.cos(angle.T), np.sin(angle.T)], axis=1) / ext
    flip = np.eye(tile // 2)[::-1].astype(ml_dtypes.bfloat16)
    high, middle, low = pieces_of(back_rows)
    rows6 = np.concatenate([high, high, middle, high, middle, low], axis=1)
    high, middle, low = pieces_of(back_cols)
    cols6 = np.concatenate([high, high, middle, high, middle, low], axis=0)
    return (
        np.concatenate(pieces_of(forward), axis=0),
        np.concatenate(pieces_of(across), axis=0),
        np.concatenate([expand] * 3, axis=1).astype(ml_dtypes.bfloat16),
        rows6,
        cols6,
        np.concatenate([flip] * 3, axis=1),
        np.concatenate([flip] * 3, axis=0),
    )


def split(value):
    high = value.astype(BF16)
    low = (value - high.astype(F32)).astype(BF16)
    return high, low


def split3(value):
    high = value.astype(BF16)
    rest = value - high.astype(F32)
    middle = rest.astype(BF16)
    low = (rest - middle.astype(F32)).astype(BF16)
    return high, middle, low


def dot(left, right):
    return jnp.dot(left, right, preferred_element_type=F32)


def strip_sum(row_start, col_start, frag_len, orient, shift, extent):
    lower = jnp.minimum(shift, 0)
    upper = jnp.maximum(shift, 0)
    along = orient == 0
    row_low = jnp.where(along, row_start, row_start + lower)
    row_high = jnp.where(along, row_start + frag_len, row_start + upper)
    col_low = jnp.where(along, col_start + lower, col_start)
    col_high = jnp.where(along, col_start + upper, col_start + frag_len)
    position = lax.broadcasted_iota(jnp.int32, (extent, shift.shape[1]), 0)
    signs = jnp.where(shift > 0, 1.0, jnp.where(shift < 0, -1.0, 0.0))
    row_select = jnp.where((position >= row_low) & (position < row_high), signs, 0.0).astype(BF16)
    col_select = jnp.where((position >= col_low) & (position < col_high), 1.0, 0.0).astype(BF16)
    return lax.dot_general(
        row_select, col_select, (((1,), (1,)), ((), ())), preferred_element_type=F32
    )


def kernel(sizes, *refs):
    away, outs = refs[:OPERANDS], refs[OPERANDS : OPERANDS + 4]
    here, rest = refs[OPERANDS + 4 : 2 * OPERANDS + 4], refs[2 * OPERANDS + 4 :]
    sems = rest[-1]
    copies = [
        pltpu.make_async_copy(src, dst, sems.at[i]) for i, (src, dst) in enumerate(zip(away, here))
    ]

    def need(*numbers):
        for number in numbers:
            copies[number].wait()

    def start(*numbers):
        for number in numbers:
            copies[number].start()

    body(sizes, start, need, away[8], *here, *outs, *rest[:-1])


def body(
    sizes,
    begin,
    need,
    spec_away,
    mask_ref,
    frow_ref,
    fcol_ref,
    flen_ref,
    fori_ref,
    fmove_ref,
    srow_ref,
    scol_ref,
    spec_ref,
    weight_ref,
    tol_ref,
    forward_ref,
    across_ref,
    expand_ref,
    rows_ref,
    cols_ref,
    flip_wide_ref,
    flip_tall_ref,
    intensity_ref,
    mask_out_ref,
    errors_ref,
    stats_ref,
    ext,
    hext,
    spec_rx,
    wv,
    wv_rx,
    sbuf,
    folded,
    choose,
    img,
    img_rx,
    err,
    err_rx,
    stat,
    stat_rx,
    halo_send,
    halo_recv,
    ka_send,
    ka_recv,
    stat_send,
    stat_recv,
    token,
):
    n_tx, n_ty, n_ka = sizes
    count = n_tx * n_ty * n_ka
    tile = mask_ref.shape[0]
    wide = ext.shape[1]
    sites = srow_ref.shape[2]
    kernels = spec_ref.shape[0]
    group = lax.axis_index("groups")
    tx = lax.axis_index("tx")
    ty = lax.axis_index("ty")
    ka = lax.axis_index("ka")
    me = (tx * n_ty + ty) * n_ka + ka

    def place(number):
        return (
            group,
            lax.div(number, n_ty * n_ka),
            lax.rem(lax.div(number, n_ka), n_ty),
            lax.rem(number, n_ka),
        )

    def remote(src, dst, send, recv, target):
        return pltpu.make_async_remote_copy(
            src_ref=src, dst_ref=dst, send_sem=send, recv_sem=recv, device_id=target, device_id_type=MESH
        )

    begin(1, 2, 3, 4, 5, 0, 9, 11, 12, 8, 13, 14, 15, 16, 17, 6, 7, 10)
    barrier = pltpu.get_barrier_semaphore()

    partner = (group, tx, ty, 1 - ka)
    up = (group, tx - 1, ty, ka)
    down = (group, tx + 1, ty, ka)
    left = (group, tx, ty - 1, ka)
    right = (group, tx, ty + 1, ka)
    around = ((tx > 0, up), (tx < n_tx - 1, down), (ty > 0, left), (ty < n_ty - 1, right))

    def signal(semaphore, target):
        pl.semaphore_signal(semaphore, inc=1, device_id=target, device_id_type=MESH)

    signal(barrier, partner)
    for there, target in around:
        pl.when(there)(functools.partial(signal, barrier, target))

    need(1, 2, 3, 4, 5, 0)
    fragments = (frow_ref[0], fcol_ref[0], flen_ref[0], fori_ref[0])
    early = lax.div(n_ty - 1 - ty, max(n_ty - 1, 1))
    halves = (early, 1 - early)

    def to_up(half):
        return remote(
            ext.at[half, pl.ds(HALO, HALO)],
            ext.at[half, pl.ds(HALO + tile, HALO)],
            halo_send.at[half],
            halo_recv.at[half],
            up,
        )

    def to_down(half):
        return remote(
            ext.at[half, pl.ds(tile, HALO)],
            ext.at[half, pl.ds(0, HALO)],
            halo_send.at[2 + half],
            halo_recv.at[2 + half],
            down,
        )

    def chain(hop, at, count_at, before, after, previous, following):
        if 0 < hop:
            pl.when(at == hop)(lambda: pl.semaphore_wait(token.at[before], 1))
            pl.when(at == count_at - 1 - hop)(lambda: pl.semaphore_wait(token.at[after], 1))
        if hop < count_at - 1:
            pl.when(at == hop)(lambda: signal(token.at[before], following))
            pl.when(at == count_at - 1 - hop)(lambda: signal(token.at[after], previous))

    def pass_across(hop):
        chain(hop, ty, n_ty, 0, 1, left, right)

    def pass_on(hop):
        chain(hop, tx, n_tx, 2, 3, up, down)

    def send_rows():
        for half in halves:
            pl.when(tx > 0)(lambda: to_up(half).start())
            pl.when(tx < n_tx - 1)(lambda: to_down(half).start())

    def place_rows(values):
        for half in range(2):
            ext[half, HALO : HALO + tile, :] = values[:, half * HALO : (half + 1) * HALO]

    first = jnp.clip(mask_ref[...] + strip_sum(*fragments, fmove_ref[0, 0, 0:1, :], tile), 0.0, 1.0)
    second = jnp.clip(first + strip_sum(*fragments, fmove_ref[0, 0, 1:2, :], tile), 0.0, 1.0)
    mask_out_ref[...] = second
    place_rows(jnp.where(ka == 0, first, second))

    peers = 1
    for at, count_at in ((tx, n_tx), (ty, n_ty)):
        for steps in (at, count_at - 1 - at):
            peers = peers + lax.div(steps + count_at - 1, count_at)
    pl.semaphore_wait(barrier, peers)

    send_rows()
    pass_across(0)

    need(9)
    for k in range(kernels):
        wv[k : k + 1, :] = jnp.full((1, 128), weight_ref[k], F32)

    to_spec = remote(spec_away, spec_rx, ka_send.at[0], ka_recv.at[0], partner)
    to_wv = remote(wv, wv_rx, ka_send.at[1], ka_recv.at[1], partner)
    to_spec.start()
    to_wv.start()

    need(7)
    position = lax.broadcasted_iota(jnp.int32, (tile, CHUNK), 0)
    for start in range(0, sites, CHUNK):
        at_cols = scol_ref[0, :, start : start + CHUNK]
        choose[:, start : start + CHUNK] = jnp.where(position == at_cols, 1.0, 0.0).astype(BF16)

    @pl.when(tx == 0)
    def _():
        ext[:, 0:HALO, :] = jnp.zeros((2, HALO, HALO), F32)

    @pl.when(tx == n_tx - 1)
    def _():
        ext[:, HALO + tile : wide, :] = jnp.zeros((2, HALO, HALO), F32)

    @pl.when(ty == 0)
    def _():
        hext[0] = jnp.zeros(hext.shape[1:], F32)

    @pl.when(ty == n_ty - 1)
    def _():
        hext[3] = jnp.zeros(hext.shape[1:], F32)

    rows = hext.shape[1]
    need(11)
    to_left = remote(hext.at[1], hext.at[3], halo_send.at[4], halo_recv.at[4], left)
    to_right = remote(hext.at[2], hext.at[0], halo_send.at[5], halo_recv.at[5], right)
    for half in halves:
        pl.when(tx > 0)(lambda: to_down(half).wait_recv())
        pl.when(tx < n_tx - 1)(lambda: to_up(half).wait_recv())
        high, middle, low = split3(ext[half])
        by = dot(forward_ref[...], jnp.concatenate([high, middle], axis=1))
        by_high, by_middle = by[:, :HALO], by[:, HALO:]
        by_low = dot(forward_ref[0:rows, :], low)
        total = (by_low + by_high[2 * rows :] + by_middle[rows : 2 * rows]) + (
            by_high[rows : 2 * rows] + by_middle[:rows]
        )
        hext[1 + half] = total + by_high[:rows]
        pl.when((half == 0) & (ty > 0))(to_left.start)
        pl.when((half == 1) & (ty < n_ty - 1))(to_right.start)

    for hop in range(1, n_ty):
        pass_across(hop)
    pass_on(0)

    @pl.when(ty > 0)
    def _():
        to_right.wait_recv()

    @pl.when(ty < n_ty - 1)
    def _():
        to_left.wait_recv()

    pass_on(1)
    need(12, 13)
    whole = jnp.concatenate([hext[0], hext[1], hext[2], hext[3]], axis=1)
    high, middle, low = split3(whole)
    by_high = dot(jnp.concatenate([high, middle, low], axis=0), across_ref[0:wide, :])
    by_middle = dot(jnp.concatenate([high, middle], axis=0), across_ref[wide : 2 * wide, :])
    by_low = dot(high, across_ref[2 * wide :, :])
    full = (by_low + by_high[2 * rows :] + by_middle[rows:]) + (by_high[rows : 2 * rows] + by_middle[:rows])
    full = full + by_high[:rows]
    full = jnp.concatenate([full, jnp.zeros((2 * BAND - rows, 2 * BAND), F32)], axis=0)
    mixed = dot(expand_ref[...], jnp.concatenate(split3(full), axis=0))
    sbuf[0] = mixed[:BAND, :BAND] - mixed[BAND:, BAND:]
    sbuf[1] = -(mixed[BAND:, :BAND] + mixed[:BAND, BAND:])

    mid = tile // 2
    folded[...] = jnp.zeros_like(folded)

    def kernel_image(spectra, scales, k):
        scale = jnp.sqrt(scales[pl.ds(k, 1), :])
        k_re = spectra[k, 0] * scale
        k_im = spectra[k, 1] * scale
        s_re = sbuf[0]
        s_im = sbuf[1]
        p_re = k_re * s_re - k_im * s_im
        p_im = k_re * s_im + k_im * s_re
        high, middle, low = split3(jnp.concatenate([p_re, p_im], axis=1))
        parts = dot(
            rows_ref[...], jnp.concatenate([high, middle, high, low, middle, high], axis=0)
        )
        even_re, even_im = parts[:mid, :BAND], parts[:mid, BAND:]
        odd_re, odd_im = parts[mid:, :BAND], parts[mid:, BAND:]
        inner = jnp.concatenate(
            [even_re - odd_im, even_re + odd_im, even_im + odd_re, even_im - odd_re], axis=0
        )
        high, middle, low = split3(inner)
        turned = dot(
            jnp.concatenate([high, middle, high, low, middle, high], axis=1), cols_ref[...]
        )
        re_cos, re_sin = turned[:tile, :mid], turned[:tile, mid:]
        im_cos, im_sin = turned[tile:, :mid], turned[tile:, mid:]
        f_re, f_im = re_cos - im_sin, im_cos + re_sin
        near = f_re * f_re + f_im * f_im
        f_re, f_im = re_cos + im_sin, im_cos - re_sin
        return near, f_re * f_re + f_im * f_im

    def add_pair(spectra, scales, k):
        near_a, far_a = kernel_image(spectra, scales, 4 * k)
        near_b, far_b = kernel_image(spectra, scales, 4 * k + 1)
        near_c, far_c = kernel_image(spectra, scales, 4 * k + 2)
        near_d, far_d = kernel_image(spectra, scales, 4 * k + 3)
        folded[:, :mid] += (near_a + near_b) + (near_c + near_d)
        folded[:, mid:] += (far_a + far_b) + (far_c + far_d)

    def add_one(spectra, scales, k):
        near, far = kernel_image(spectra, scales, k)
        folded[:, :mid] += near
        folded[:, mid:] += far

    def own_step(k, carry):
        add_pair(spec_ref, wv, k)
        return carry

    def rx_step(k, carry):
        add_pair(spec_rx, wv_rx, k)
        return carry

    need(8, 14, 15)
    lax.fori_loop(0, kernels // 4, own_step, 0)
    for k in range(kernels // 4 * 4, kernels):
        add_one(spec_ref, wv, k)
    pass_on(2)
    to_spec.wait_recv()
    to_wv.wait_recv()
    lax.fori_loop(0, kernels // 4, rx_step, 0)
    for k in range(kernels // 4 * 4, kernels):
        add_one(spec_rx, wv_rx, k)

    for hop in range(3, n_tx):
        pass_on(hop)
    need(16, 17)
    lower = jnp.concatenate(split3(folded[mid:, :]), axis=0)
    ordered = jnp.concatenate([dot(flip_wide_ref[...], lower), folded[:mid, :]], axis=0)
    lower = jnp.concatenate(split3(ordered[:, mid:]), axis=1)
    img[...] = jnp.concatenate([dot(lower, flip_tall_ref[...]), ordered[:, :mid]], axis=1)
    to_img = remote(img, img_rx, ka_send.at[2], ka_recv.at[2], partner)
    to_img.start()

    image = img[...]
    grad_rows = (pltpu.roll(image, tile - 1, 0) - pltpu.roll(image, 1, 0)) * 0.5
    grad_cols = (pltpu.roll(image, tile - 1, 1) - pltpu.roll(image, 1, 1)) * 0.5
    slope = jnp.sqrt(grad_rows * grad_rows + grad_cols * grad_cols)
    error_map = (image - LEVEL) / jnp.maximum(slope, SLOPE_FLOOR)
    high, low = split(error_map)
    need(6, 10)
    limit = tol_ref[ka].astype(F32) / 8.0
    peak = jnp.zeros((1, CHUNK), F32)
    total = jnp.zeros((1, CHUNK), F32)
    for start in range(0, sites, CHUNK):
        at_rows = srow_ref[0, :, start : start + CHUNK]
        picked = dot(high, choose[:, start : start + CHUNK]) + dot(low, choose[:, start : start + CHUNK])
        errors = jnp.sum(jnp.where(position == at_rows, picked, 0.0), axis=0, keepdims=True)
        err[:, start : start + CHUNK] = errors
        size = jnp.abs(errors)
        peak = jnp.maximum(peak, size)
        total = total + 1.0 / (1.0 + jnp.exp(-SHARPNESS * (limit - size)))
    stat[0:1, :] = functools.reduce(
        jnp.maximum, [peak[:, i : i + 128] for i in range(0, CHUNK, 128)]
    )
    stat[1:2, :] = functools.reduce(
        jnp.add, [total[:, i : i + 128] for i in range(0, CHUNK, 128)]
    )
    to_err = remote(err, err_rx, ka_send.at[3], ka_recv.at[3], partner)
    to_err.start()

    def to_stat(offset):
        return remote(
            stat,
            stat_rx.at[me],
            stat_send.at[offset],
            stat_recv.at[me],
            place(lax.rem(me + offset, count)),
        )

    def send_stat(offset, carry):
        to_stat(offset).start()
        return carry

    lax.fori_loop(1, count, send_stat, 0)
    stat_rx[pl.ds(me, 1)] = stat[...][None]

    to_img.wait_recv()
    intensity_ref[...] = jnp.where(ka == ITERS - 1, image, img_rx[...])
    to_err.wait_recv()
    mine = err[...]
    theirs = err_rx[...]
    errors_ref[0, 0, 0:1, :] = jnp.where(ka == 0, mine, theirs)
    errors_ref[0, 0, 1:2, :] = jnp.where(ka == 0, theirs, mine)

    def wait_stat(offset, carry):
        to_stat(offset).wait_send()
        source = lax.rem(me + offset, count)
        remote(
            stat, stat_rx.at[source], stat_send.at[offset], stat_recv.at[source], place(source)
        ).wait_recv()
        return carry

    lax.fori_loop(1, count, wait_stat, 0)

    for which in range(ITERS):
        rows_of = range(which, count, n_ka)
        stats_ref[which : which + 1, :] = functools.reduce(
            jnp.maximum, [stat_rx[number, 0:1, :] for number in rows_of]
        )
        stats_ref[ITERS + which : ITERS + which + 1, :] = functools.reduce(
            jnp.add, [stat_rx[number, 1:2, :] for number in rows_of]
        )

    for half in range(2):
        pl.when(tx > 0)(lambda: to_up(half).wait_send())
        pl.when(tx < n_tx - 1)(lambda: to_down(half).wait_send())

    @pl.when(ty > 0)
    def _():
        to_left.wait_send()

    @pl.when(ty < n_ty - 1)
    def _():
        to_right.wait_send()

    for copy in (to_spec, to_wv, to_img, to_err):
        copy.wait_send()


def write(scale, image, mask, errors, stats, image_out, mask_out, errors_out, peaks, shares, sems):
    copies = [
        pltpu.make_async_copy(src, dst, sems.at[i])
        for i, (src, dst) in enumerate(((image, image_out), (mask, mask_out), (errors, errors_out)))
    ]
    for copy in copies:
        copy.start()
    for i in range(ITERS):
        peaks[i] = jnp.max(stats[i : i + 1, :])
        shares[i] = jnp.sum(stats[ITERS + i : ITERS + i + 1, :]) * scale
    for copy in copies:
        copy.wait()


def shards(sizes, *args):
    mask_raster, spectra = args[0], args[8]
    site_count = args[6].shape[2]
    tile = mask_raster.shape[0]
    wide = tile + 2 * HALO
    consts = [jnp.asarray(a) for a in tables(tile)]
    rows = consts[0].shape[0] // 3
    kernels = spectra.shape[0]
    count = sizes[0] * sizes[1] * sizes[2]
    vmem = pl.BlockSpec(memory_space=pltpu.VMEM)
    smem = pl.BlockSpec(memory_space=pltpu.SMEM)
    dma = pltpu.SemaphoreType.DMA
    operands = tuple(
        pltpu.with_memory_space_constraint(a, pltpu.HBM) for a in (*args, *consts)
    )
    local = [
        (pltpu.SMEM if number in (9, 10) else pltpu.VMEM)(a.shape, a.dtype)
        for number, a in enumerate(operands)
    ]
    tile_shape = (tile, tile)
    error_shape = (1, 1, ITERS, site_count)
    results = pl.pallas_call(
            functools.partial(kernel, sizes),
            out_shape=(
                pltpu.VMEM(tile_shape, F32),
                pltpu.VMEM(tile_shape, F32),
                pltpu.VMEM(error_shape, F32),
                pltpu.VMEM((8, 128), F32),
            ),
            in_specs=[pl.BlockSpec(memory_space=pltpu.HBM)] * OPERANDS,
            out_specs=(vmem,) * 4,
            scratch_shapes=local
            + [
                pltpu.VMEM((2, wide, HALO), F32),
                pltpu.VMEM((4, rows, HALO), F32),
                pltpu.VMEM(spectra.shape, F32),
                pltpu.VMEM((kernels, 128), F32),
                pltpu.VMEM((kernels, 128), F32),
                pltpu.VMEM((2, BAND, BAND), F32),
                pltpu.VMEM((tile, tile), F32),
                pltpu.VMEM((tile, site_count), BF16),
                pltpu.VMEM((tile, tile), F32),
                pltpu.VMEM((tile, tile), F32),
                pltpu.VMEM((1, site_count), F32),
                pltpu.VMEM((1, site_count), F32),
                pltpu.VMEM((2, 128), F32),
                pltpu.VMEM((count, 2, 128), F32),
                dma((6,)),
                dma((6,)),
                dma((4,)),
                dma((4,)),
                dma((count,)),
                dma((count,)),
                pltpu.SemaphoreType.REGULAR((4,)),
                dma((OPERANDS,)),
            ],
            compiler_params=pltpu.CompilerParams(
                collective_id=0, has_side_effects=True, vmem_limit_bytes=VMEM_LIMIT
            ),
        )(*operands)
    hbm = pl.BlockSpec(memory_space=pltpu.HBM)
    return tuple(
        pl.pallas_call(
            functools.partial(write, 1.0 / (site_count * sizes[0] * sizes[1])),
            out_shape=(
                jax.ShapeDtypeStruct(tile_shape, F32),
                jax.ShapeDtypeStruct(tile_shape, F32),
                jax.ShapeDtypeStruct(error_shape, F32),
                jax.ShapeDtypeStruct((ITERS,), F32),
                jax.ShapeDtypeStruct((ITERS,), F32),
            ),
            in_specs=[vmem] * 4,
            out_specs=(hbm, hbm, hbm, smem, smem),
            scratch_shapes=[dma((3,))],
            compiler_params=pltpu.CompilerParams(vmem_limit_bytes=VMEM_LIMIT),
        )(*results)
    )


def solution(mesh):
    sizes = tuple(mesh.shape[axis] for axis in ("tx", "ty", "ka"))
    assert sizes[2] == ITERS
    placed = (
        P(("groups", "tx"), "ty"),
        P(("groups", "tx"), "ty", None),
        P(("groups", "tx"), "ty", None),
        P(("groups", "tx"), "ty", None),
        P(("groups", "tx"), "ty", None),
        P(("groups", "tx"), "ty", None, None),
        P(("groups", "tx"), "ty", None),
        P(("groups", "tx"), "ty", None),
        P("ka", None, None, None),
        P("ka"),
        P(),
    )
    return jax.shard_map(
        functools.partial(shards, sizes),
        mesh=mesh,
        in_specs=placed,
        out_specs=(
            P(("groups", "tx"), "ty"),
            P(("groups", "tx"), "ty"),
            P(("groups", "tx"), "ty", None, None),
            P("groups"),
            P("groups"),
        ),
        check_vma=False,
    )
```

```python
import functools
import math

import jax
import jax.numpy as jnp
import ml_dtypes
import numpy as np
from jax import lax
from jax.experimental import pallas as pl
from jax.experimental.pallas import tpu as pltpu
from jax.sharding import PartitionSpec as P

HALO = 128
BAND = 128
ITERS = 2

LEVEL = 0.4
SLOPE_FLOOR = 0.05
SHARPNESS = 8.0
CHUNK = 256
ROWS = 32
OPERANDS = 19
VMEM_LIMIT = 32 * 1024 * 1024
MESH = pl.DeviceIdType.MESH
F32 = jnp.float32
BF16 = jnp.bfloat16


def pieces_of(table):
    high = table.astype(ml_dtypes.bfloat16)
    rest = table - high.astype(np.float64)
    middle = rest.astype(ml_dtypes.bfloat16)
    low = (rest - middle.astype(np.float64)).astype(ml_dtypes.bfloat16)
    return high, middle, low


def tables(tile):
    ext = tile + 2 * HALO
    half = BAND // 2
    step = 2.0 * math.pi / ext
    rows = -(-(2 * half + 1) // 16) * 16
    span = np.arange(ext) - (ext - 1) / 2
    positive = np.arange(half + 1)
    freq = np.arange(BAND) - half
    forward = np.zeros((rows, ext))
    forward[: half + 1] = np.cos(step * positive[:, None] * span[None])
    forward[half + 1 : 2 * half + 1] = np.sin(step * positive[1:, None] * span[None])
    pairs = np.arange(half)
    phase = step * span[:, None] * np.concatenate([pairs, -1 - pairs])[None]
    across = np.concatenate([np.cos(phase), np.sin(phase)], axis=1)
    across = np.concatenate([across[HALO:-HALO], across[:HALO], across[-HALO:]], axis=0)
    expand = np.zeros((2 * BAND, 2 * BAND))
    for place, number in enumerate(freq):
        expand[place, abs(number)] = 1.0
        if number != 0:
            expand[BAND + place, half + abs(number)] = np.sign(number)
    pixels = np.arange(tile // 2) + 0.5
    angle = step * pixels[:, None] * (freq[None] + 0.5)
    back_rows = np.concatenate([np.cos(angle), np.sin(angle)], axis=0) / ext
    angle = step * (pairs[:, None] + 0.5) * pixels[None]
    turn = np.eye(half)[::-1]
    turn = np.block([[turn, 0 * turn], [0 * turn, turn]]).astype(ml_dtypes.bfloat16)
    flip = np.eye(tile // 2)[::-1].astype(ml_dtypes.bfloat16)
    high, middle, low = pieces_of(back_rows)
    rows6 = np.concatenate([high, high, middle, high, middle, low], axis=1)
    cols6 = []
    for wave in (np.cos(angle), np.sin(angle)):
        high, middle, low = pieces_of(wave / ext)
        none = np.zeros_like(high)
        cols6.append(np.concatenate([high, high, high, low], axis=0))
        cols6.append(np.concatenate([middle, middle, none, none], axis=0))
    cols6 = np.concatenate(
        [np.concatenate(cols6[:2], axis=1), np.concatenate(cols6[2:], axis=1)], axis=0
    )
    return (
        np.concatenate(pieces_of(forward), axis=0),
        np.concatenate(pieces_of(across), axis=0),
        np.concatenate([expand] * 3, axis=1).astype(ml_dtypes.bfloat16),
        rows6,
        cols6,
        np.concatenate([flip] * 3, axis=1),
        np.concatenate([flip] * 3, axis=0),
        np.concatenate([turn] * 3, axis=0),
    )


def split(value):
    high = value.astype(BF16)
    low = (value - high.astype(F32)).astype(BF16)
    return high, low


def split3(value):
    high = value.astype(BF16)
    rest = value - high.astype(F32)
    middle = rest.astype(BF16)
    low = (rest - middle.astype(F32)).astype(BF16)
    return high, middle, low


def dot(left, right):
    return jnp.dot(left, right, preferred_element_type=F32)


def strip_sum(row_start, col_start, frag_len, orient, shift, extent):
    lower = jnp.minimum(shift, 0)
    upper = jnp.maximum(shift, 0)
    along = orient == 0
    row_low = jnp.where(along, row_start, row_start + lower)
    row_high = jnp.where(along, row_start + frag_len, row_start + upper)
    col_low = jnp.where(along, col_start + lower, col_start)
    col_high = jnp.where(along, col_start + upper, col_start + frag_len)
    position = lax.broadcasted_iota(jnp.int32, (extent, shift.shape[1]), 0)
    signs = jnp.where(shift > 0, 1.0, jnp.where(shift < 0, -1.0, 0.0))
    row_select = jnp.where((position >= row_low) & (position < row_high), signs, 0.0).astype(BF16)
    col_select = jnp.where((position >= col_low) & (position < col_high), 1.0, 0.0).astype(BF16)
    return lax.dot_general(
        row_select, col_select, (((1,), (1,)), ((), ())), preferred_element_type=F32
    )


def kernel(sizes, *refs):
    away, outs = refs[:OPERANDS], refs[OPERANDS : OPERANDS + 4]
    here, rest = refs[OPERANDS + 4 : 2 * OPERANDS + 4], refs[2 * OPERANDS + 4 :]
    sems = rest[-1]
    copies = [
        pltpu.make_async_copy(src, dst, sems.at[i]) for i, (src, dst) in enumerate(zip(away, here))
    ]

    def need(*numbers):
        for number in numbers:
            copies[number].wait()

    def start(*numbers):
        for number in numbers:
            copies[number].start()

    body(sizes, start, need, *here, *outs, *rest[:-1])


def body(
    sizes,
    begin,
    need,
    mask_ref,
    frow_ref,
    fcol_ref,
    flen_ref,
    fori_ref,
    fmove_ref,
    srow_ref,
    scol_ref,
    spec_ref,
    weight_ref,
    tol_ref,
    forward_ref,
    across_ref,
    expand_ref,
    rows_ref,
    cols_ref,
    flip_wide_ref,
    flip_tall_ref,
    turn_ref,
    intensity_ref,
    mask_out_ref,
    errors_ref,
    stats_ref,
    ext,
    hext,
    paired,
    stacked_a,
    stacked_b,
    sbuf,
    folded,
    choose,
    img,
    img_rx,
    err,
    err_rx,
    stat,
    stat_rx,
    halo_send,
    halo_recv,
    ka_send,
    ka_recv,
    stat_send,
    stat_recv,
    token,
):
    n_tx, n_ty, n_ka = sizes
    count = n_tx * n_ty * n_ka
    tile = mask_ref.shape[0]
    wide = ext.shape[1]
    sites = srow_ref.shape[2]
    kernels = spec_ref.shape[0]
    group = lax.axis_index("groups")
    tx = lax.axis_index("tx")
    ty = lax.axis_index("ty")
    ka = lax.axis_index("ka")
    me = (tx * n_ty + ty) * n_ka + ka

    def place(number):
        return (
            group,
            lax.div(number, n_ty * n_ka),
            lax.rem(lax.div(number, n_ka), n_ty),
            lax.rem(number, n_ka),
        )

    def remote(src, dst, send, recv, target):
        return pltpu.make_async_remote_copy(
            src_ref=src, dst_ref=dst, send_sem=send, recv_sem=recv, device_id=target, device_id_type=MESH
        )

    begin(1, 2, 3, 4, 5, 0, 9, 7, 18, 8, 11, 12, 13, 14, 15, 6, 10, 16, 17)
    barrier = pltpu.get_barrier_semaphore()

    partner = (group, tx, ty, 1 - ka)
    up = (group, tx - 1, ty, ka)
    down = (group, tx + 1, ty, ka)
    left = (group, tx, ty - 1, ka)
    right = (group, tx, ty + 1, ka)
    around = ((tx > 0, up), (tx < n_tx - 1, down), (ty > 0, left), (ty < n_ty - 1, right))

    def signal(semaphore, target):
        pl.semaphore_signal(semaphore, inc=1, device_id=target, device_id_type=MESH)

    signal(barrier, partner)
    for there, target in around:
        pl.when(there)(functools.partial(signal, barrier, target))

    need(1, 2, 3, 4, 5, 0)
    fragments = (frow_ref[0], fcol_ref[0], flen_ref[0], fori_ref[0])
    early = lax.div(n_ty - 1 - ty, max(n_ty - 1, 1))
    halves = (early, 1 - early)

    def to_up(half):
        return remote(
            ext.at[half, pl.ds(HALO, HALO)],
            ext.at[half, pl.ds(HALO + tile, HALO)],
            halo_send.at[half],
            halo_recv.at[half],
            up,
        )

    def to_down(half):
        return remote(
            ext.at[half, pl.ds(tile, HALO)],
            ext.at[half, pl.ds(0, HALO)],
            halo_send.at[2 + half],
            halo_recv.at[2 + half],
            down,
        )

    def chain(hop, at, count_at, before, after, previous, following):
        if 0 < hop:
            pl.when(at == hop)(lambda: pl.semaphore_wait(token.at[before], 1))
            pl.when(at == count_at - 1 - hop)(lambda: pl.semaphore_wait(token.at[after], 1))
        if hop < count_at - 1:
            pl.when(at == hop)(lambda: signal(token.at[before], following))
            pl.when(at == count_at - 1 - hop)(lambda: signal(token.at[after], previous))

    def pass_across(hop):
        chain(hop, ty, n_ty, 0, 1, left, right)

    def pass_on(hop):
        chain(hop, tx, n_tx, 2, 3, up, down)

    def send_rows():
        for half in halves:
            pl.when(tx > 0)(lambda: to_up(half).start())
            pl.when(tx < n_tx - 1)(lambda: to_down(half).start())

    def place_rows(values):
        for half in range(2):
            ext[half, HALO : HALO + tile, :] = values[:, half * HALO : (half + 1) * HALO]

    peers = 1
    for at, count_at in ((tx, n_tx), (ty, n_ty)):
        for steps in (at, count_at - 1 - at):
            peers = peers + lax.div(steps + count_at - 1, count_at)

    def send_off():
        pl.semaphore_wait(barrier, peers)
        send_rows()
        pass_across(0)

    first = jnp.clip(mask_ref[...] + strip_sum(*fragments, fmove_ref[0, 0, 0:1, :], tile), 0.0, 1.0)
    place_rows(first)
    second = jnp.clip(first + strip_sum(*fragments, fmove_ref[0, 0, 1:2, :], tile), 0.0, 1.0)
    mask_out_ref[...] = second
    pl.when(ka == 1)(lambda: place_rows(second))
    send_off()

    def fold(at):
        return jnp.where(at < tile // 2, tile - 1 - at, at - tile // 2)

    need(7)
    position = lax.broadcasted_iota(jnp.int32, (tile, CHUNK), 0)
    for start in range(0, sites, CHUNK):
        at_cols = fold(scol_ref[0, :, start : start + CHUNK])
        choose[:, start : start + CHUNK] = jnp.where(position == at_cols, 1.0, 0.0).astype(BF16)

    lower_lanes = lax.broadcasted_iota(jnp.int32, (BAND, BAND), 1) < BAND // 2

    def swap(value):
        return pltpu.roll(value, BAND // 2, 1)

    def pair(k):
        scale = jnp.sqrt(jnp.full((1, BAND), weight_ref[k], F32))
        k_re, k_im = spec_ref[k, 0], spec_ref[k, 1]
        below = jnp.where(lower_lanes, k_re, swap(k_im)) * scale
        paired[k, 0] = jnp.where(lower_lanes, swap(k_re), k_im) * scale
        paired[k, 1] = dot(jnp.concatenate(split3(below), axis=1), turn_ref[...])

    def pair_step(k, carry):
        for number in range(4):
            pair(4 * k + number)
        return carry

    need(9, 8, 18)
    lax.fori_loop(0, kernels // 4, pair_step, 0)
    for k in range(kernels // 4 * 4, kernels):
        pair(k)

    @pl.when(tx == 0)
    def _():
        ext[:, 0:HALO, :] = jnp.zeros((2, HALO, HALO), F32)

    @pl.when(tx == n_tx - 1)
    def _():
        ext[:, HALO + tile : wide, :] = jnp.zeros((2, HALO, HALO), F32)

    @pl.when(ty == 0)
    def _():
        hext[0] = jnp.zeros(hext.shape[1:], F32)

    @pl.when(ty == n_ty - 1)
    def _():
        hext[3] = jnp.zeros(hext.shape[1:], F32)

    rows = hext.shape[1]
    need(11)
    to_left = remote(hext.at[1], hext.at[3], halo_send.at[4], halo_recv.at[4], left)
    to_right = remote(hext.at[2], hext.at[0], halo_send.at[5], halo_recv.at[5], right)
    for half in halves:
        pl.when(tx > 0)(lambda: to_down(half).wait_recv())
        pl.when(tx < n_tx - 1)(lambda: to_up(half).wait_recv())
        high, middle, low = split3(ext[half])
        by = dot(forward_ref[...], jnp.concatenate([high, middle], axis=1))
        by_high, by_middle = by[:, :HALO], by[:, HALO:]
        by_low = dot(forward_ref[0:rows, :], low)
        total = (by_low + by_high[2 * rows :] + by_middle[rows : 2 * rows]) + (
            by_high[rows : 2 * rows] + by_middle[:rows]
        )
        hext[1 + half] = total + by_high[:rows]
        pl.when((half == 0) & (ty > 0))(to_left.start)
        pl.when((half == 1) & (ty < n_ty - 1))(to_right.start)

    for hop in range(1, n_ty):
        pass_across(hop)
    to_spec = remote(
        paired.at[pl.ds(0, kernels)],
        paired.at[pl.ds(kernels, kernels)],
        ka_send.at[0],
        ka_recv.at[0],
        partner,
    )
    to_spec.start()
    pass_on(0)
    need(12, 13)

    def column_part(block, first_row):
        high, middle, low = split3(block)
        depth = block.shape[1]

        def piece(number):
            return across_ref[number * wide + first_row : number * wide + first_row + depth, :]

        by_high = dot(jnp.concatenate([high, middle, low], axis=0), piece(0))
        by_middle = dot(jnp.concatenate([high, middle], axis=0), piece(1))
        by_low = dot(high, piece(2))
        part = (by_low + by_high[2 * rows :] + by_middle[rows:]) + (
            by_high[rows : 2 * rows] + by_middle[:rows]
        )
        return part + by_high[:rows]

    own_part = column_part(jnp.concatenate([hext[1], hext[2]], axis=1), 0)

    @pl.when(ty > 0)
    def _():
        to_right.wait_recv()

    @pl.when(ty < n_ty - 1)
    def _():
        to_left.wait_recv()

    pass_on(1)
    full = own_part + column_part(jnp.concatenate([hext[0], hext[3]], axis=1), tile)
    full = jnp.concatenate([full, jnp.zeros((2 * BAND - rows, 2 * BAND), F32)], axis=0)
    mixed = dot(expand_ref[...], jnp.concatenate(split3(full), axis=0))
    s_re = mixed[:BAND, :BAND] - mixed[BAND:, BAND:]
    s_im = -(mixed[BAND:, :BAND] + mixed[:BAND, BAND:])
    sbuf[0] = jnp.where(lower_lanes, s_re, swap(s_re))
    sbuf[1] = jnp.where(lower_lanes, -s_im, swap(s_im))
    sbuf[2] = jnp.where(lower_lanes, swap(s_re), s_re)
    sbuf[3] = jnp.where(lower_lanes, -swap(s_im), s_im)

    mid = tile // 2
    folded[...] = jnp.zeros_like(folded)

    low_half = lax.broadcasted_iota(jnp.int32, (tile, BAND), 1) < BAND // 2

    def first_stage(k, stacked):
        plus, minus = paired[k, 0], paired[k, 1]
        p_plus = plus * sbuf[0] + swap(plus) * sbuf[1]
        p_minus = minus * sbuf[2] + swap(minus) * sbuf[3]
        high, middle, low = split3(
            jnp.concatenate([p_plus + p_minus, p_plus - p_minus], axis=1)
        )
        inner = dot(
            rows_ref[...], jnp.concatenate([high, middle, high, low, middle, high], axis=0)
        )
        for number in range(2):
            part = inner[:, number * BAND : (number + 1) * BAND]
            high, middle, low = split3(part)
            high_turned, middle_turned, low_turned = swap(high), swap(middle), swap(low)
            blocks = (
                (jnp.where(low_half, high, middle_turned), jnp.where(low_half, low, high_turned)),
                (jnp.where(low_half, high_turned, middle), jnp.where(low_half, low_turned, high)),
            )
            for row in range(0, mid, ROWS):
                for place_in, (left_part, right_part) in enumerate(blocks):
                    for wave in range(2):
                        at = 4 * row + (2 * place_in + wave) * ROWS
                        taken = slice(wave * mid + row, wave * mid + row + ROWS)
                        stacked[number, at : at + ROWS, :BAND] = left_part[taken]
                        stacked[number, at : at + ROWS, BAND:] = right_part[taken]

    def across_part(stacked, number, row):
        turned = dot(
            stacked[number, 4 * row : 4 * (row + ROWS), :],
            cols_ref[number * tile : (number + 1) * tile, :],
        )
        whole = turned[:, :mid] + turned[:, mid:]
        return [whole[quarter * ROWS : (quarter + 1) * ROWS] for quarter in range(4)]

    def second_stage(stacked):
        for row in range(0, mid, ROWS):
            cc_re, sc_re, cc_im, sc_im = across_part(stacked, 0, row)
            cs_re, ss_re, cs_im, ss_im = across_part(stacked, 1, row)

            def both(side, x_re, x_im, y_re, y_im):
                at = (slice(row, row + ROWS), slice(side, side + mid))
                folded[at] += (x_re - y_im) * (x_re - y_im) + (x_im + y_re) * (x_im + y_re)
                at = (slice(mid + row, mid + row + ROWS), slice(mid - side, tile - side))
                folded[at] += (x_re + y_im) * (x_re + y_im) + (x_im - y_re) * (x_im - y_re)

            both(0, cc_re - ss_re, cc_im - ss_im, sc_re + cs_re, sc_im + cs_im)
            both(mid, cc_re + ss_re, cc_im + ss_im, sc_re - cs_re, sc_im - cs_im)

    stacks = (stacked_a, stacked_b)
    unroll = 4 if kernels % 2 == 0 else 2

    def some_kernels(k, carry):
        for number in range(unroll):
            following = jnp.minimum(unroll * k + number + 1, 2 * kernels - 1)
            first_stage(following, stacks[(number + 1) % 2])
            second_stage(stacks[number % 2])
        return carry

    need(14, 15)
    first_stage(0, stacked_a)
    half_way = (kernels - 1) // unroll
    lax.fori_loop(0, half_way, some_kernels, 0)
    pass_on(2)
    to_spec.wait_recv()
    lax.fori_loop(half_way, 2 * kernels // unroll, some_kernels, 0)
    for hop in range(3, n_tx):
        pass_on(hop)
    image = folded[...]

    def gradient(axis):
        along = lax.broadcasted_iota(jnp.int32, (tile, tile), axis)
        before = jnp.where(
            lax.rem(along, mid) == 0, pltpu.roll(image, mid, axis), pltpu.roll(image, 1, axis)
        )
        return (pltpu.roll(image, tile - 1, axis) - before) * 0.5

    grad_rows, grad_cols = gradient(0), gradient(1)
    slope = jnp.sqrt(grad_rows * grad_rows + grad_cols * grad_cols)
    error_map = (image - LEVEL) / jnp.maximum(slope, SLOPE_FLOOR)
    high, low = split(error_map)
    need(6, 10)
    limit = tol_ref[ka].astype(F32) / 8.0
    peak = jnp.zeros((1, CHUNK), F32)
    total = jnp.zeros((1, CHUNK), F32)
    for start in range(0, sites, CHUNK):
        at_rows = fold(srow_ref[0, :, start : start + CHUNK])
        picked = dot(high, choose[:, start : start + CHUNK]) + dot(low, choose[:, start : start + CHUNK])
        errors = jnp.sum(jnp.where(position == at_rows, picked, 0.0), axis=0, keepdims=True)
        err[:, start : start + CHUNK] = errors
        size = jnp.abs(errors)
        peak = jnp.maximum(peak, size)
        total = total + 1.0 / (1.0 + jnp.exp(-SHARPNESS * (limit - size)))
    stat[0:1, :] = functools.reduce(
        jnp.maximum, [peak[:, i : i + 128] for i in range(0, CHUNK, 128)]
    )
    stat[1:2, :] = functools.reduce(
        jnp.add, [total[:, i : i + 128] for i in range(0, CHUNK, 128)]
    )
    to_err = remote(err, err_rx, ka_send.at[3], ka_recv.at[3], partner)
    to_err.start()

    def to_stat(offset):
        return remote(
            stat,
            stat_rx.at[me],
            stat_send.at[offset],
            stat_recv.at[me],
            place(lax.rem(me + offset, count)),
        )

    def send_stat(offset, carry):
        to_stat(offset).start()
        return carry

    lax.fori_loop(1, count, send_stat, 0)
    stat_rx[pl.ds(me, 1)] = stat[...][None]

    to_img = remote(img, img_rx, ka_send.at[2], ka_recv.at[2], partner)
    need(16, 17)

    @pl.when(ka == ITERS - 1)
    def _():
        lower = jnp.concatenate(split3(folded[mid:, :]), axis=0)
        ordered = jnp.concatenate([dot(flip_wide_ref[...], lower), folded[:mid, :]], axis=0)
        lower = jnp.concatenate(split3(ordered[:, mid:]), axis=1)
        result = jnp.concatenate([dot(lower, flip_tall_ref[...]), ordered[:, :mid]], axis=1)
        img[...] = result
        to_img.start()
        intensity_ref[...] = result

    @pl.when(ka < ITERS - 1)
    def _():
        to_img.wait_recv()
        intensity_ref[...] = img_rx[...]

    to_err.wait_recv()
    mine = err[...]
    theirs = err_rx[...]
    errors_ref[0, 0, 0:1, :] = jnp.where(ka == 0, mine, theirs)
    errors_ref[0, 0, 1:2, :] = jnp.where(ka == 0, theirs, mine)

    def wait_stat(offset, carry):
        to_stat(offset).wait_send()
        source = lax.rem(me + offset, count)
        remote(
            stat, stat_rx.at[source], stat_send.at[offset], stat_recv.at[source], place(source)
        ).wait_recv()
        return carry

    lax.fori_loop(1, count, wait_stat, 0)

    for which in range(ITERS):
        rows_of = range(which, count, n_ka)
        stats_ref[which : which + 1, :] = functools.reduce(
            jnp.maximum, [stat_rx[number, 0:1, :] for number in rows_of]
        )
        stats_ref[ITERS + which : ITERS + which + 1, :] = functools.reduce(
            jnp.add, [stat_rx[number, 1:2, :] for number in rows_of]
        )

    for half in range(2):
        pl.when(tx > 0)(lambda: to_up(half).wait_send())
        pl.when(tx < n_tx - 1)(lambda: to_down(half).wait_send())

    @pl.when(ty > 0)
    def _():
        to_left.wait_send()

    @pl.when(ty < n_ty - 1)
    def _():
        to_right.wait_send()

    pl.when(ka == ITERS - 1)(to_img.wait_send)
    for copy in (to_spec, to_err):
        copy.wait_send()


def write(scale, image, mask, errors, stats, image_out, mask_out, errors_out, peaks, shares, sems):
    copies = [
        pltpu.make_async_copy(src, dst, sems.at[i])
        for i, (src, dst) in enumerate(((image, image_out), (mask, mask_out), (errors, errors_out)))
    ]
    for copy in copies:
        copy.start()
    for i in range(ITERS):
        peaks[i] = jnp.max(stats[i : i + 1, :])
        shares[i] = jnp.sum(stats[ITERS + i : ITERS + i + 1, :]) * scale
    for copy in copies:
        copy.wait()


def shards(sizes, *args):
    mask_raster, spectra = args[0], args[8]
    site_count = args[6].shape[2]
    tile = mask_raster.shape[0]
    wide = tile + 2 * HALO
    consts = [jnp.asarray(a) for a in tables(tile)]
    rows = consts[0].shape[0] // 3
    kernels = spectra.shape[0]
    count = sizes[0] * sizes[1] * sizes[2]
    vmem = pl.BlockSpec(memory_space=pltpu.VMEM)
    smem = pl.BlockSpec(memory_space=pltpu.SMEM)
    dma = pltpu.SemaphoreType.DMA
    operands = tuple(
        pltpu.with_memory_space_constraint(a, pltpu.HBM) for a in (*args, *consts)
    )
    local = [
        (pltpu.SMEM if number in (9, 10) else pltpu.VMEM)(a.shape, a.dtype)
        for number, a in enumerate(operands)
    ]
    tile_shape = (tile, tile)
    error_shape = (1, 1, ITERS, site_count)
    results = pl.pallas_call(
            functools.partial(kernel, sizes),
            out_shape=(
                pltpu.VMEM(tile_shape, F32),
                pltpu.VMEM(tile_shape, F32),
                pltpu.VMEM(error_shape, F32),
                pltpu.VMEM((8, 128), F32),
            ),
            in_specs=[pl.BlockSpec(memory_space=pltpu.HBM)] * OPERANDS,
            out_specs=(vmem,) * 4,
            scratch_shapes=local
            + [
                pltpu.VMEM((2, wide, HALO), F32),
                pltpu.VMEM((4, rows, HALO), F32),
                pltpu.VMEM((2 * kernels, *spectra.shape[1:]), F32),
                pltpu.VMEM((2, 2 * tile, tile), BF16),
                pltpu.VMEM((2, 2 * tile, tile), BF16),
                pltpu.VMEM((4, BAND, BAND), F32),
                pltpu.VMEM((tile, tile), F32),
                pltpu.VMEM((tile, site_count), BF16),
                pltpu.VMEM((tile, tile), F32),
                pltpu.VMEM((tile, tile), F32),
                pltpu.VMEM((1, site_count), F32),
                pltpu.VMEM((1, site_count), F32),
                pltpu.VMEM((2, 128), F32),
                pltpu.VMEM((count, 2, 128), F32),
                dma((6,)),
                dma((6,)),
                dma((4,)),
                dma((4,)),
                dma((count,)),
                dma((count,)),
                pltpu.SemaphoreType.REGULAR((4,)),
                dma((OPERANDS,)),
            ],
            compiler_params=pltpu.CompilerParams(
                collective_id=0, has_side_effects=True, vmem_limit_bytes=VMEM_LIMIT
            ),
        )(*operands)
    hbm = pl.BlockSpec(memory_space=pltpu.HBM)
    return tuple(
        pl.pallas_call(
            functools.partial(write, 1.0 / (site_count * sizes[0] * sizes[1])),
            out_shape=(
                jax.ShapeDtypeStruct(tile_shape, F32),
                jax.ShapeDtypeStruct(tile_shape, F32),
                jax.ShapeDtypeStruct(error_shape, F32),
                jax.ShapeDtypeStruct((ITERS,), F32),
                jax.ShapeDtypeStruct((ITERS,), F32),
            ),
            in_specs=[vmem] * 4,
            out_specs=(hbm, hbm, hbm, smem, smem),
            scratch_shapes=[dma((3,))],
            compiler_params=pltpu.CompilerParams(vmem_limit_bytes=VMEM_LIMIT),
        )(*results)
    )


def solution(mesh):
    sizes = tuple(mesh.shape[axis] for axis in ("tx", "ty", "ka"))
    assert sizes[2] == ITERS
    placed = (
        P(("groups", "tx"), "ty"),
        P(("groups", "tx"), "ty", None),
        P(("groups", "tx"), "ty", None),
        P(("groups", "tx"), "ty", None),
        P(("groups", "tx"), "ty", None),
        P(("groups", "tx"), "ty", None, None),
        P(("groups", "tx"), "ty", None),
        P(("groups", "tx"), "ty", None),
        P("ka", None, None, None),
        P("ka"),
        P(),
    )
    return jax.shard_map(
        functools.partial(shards, sizes),
        mesh=mesh,
        in_specs=placed,
        out_specs=(
            P(("groups", "tx"), "ty"),
            P(("groups", "tx"), "ty"),
            P(("groups", "tx"), "ty", None, None),
            P("groups"),
            P("groups"),
        ),
        check_vma=False,
    )
```

```python
import functools
import math

import jax
import jax.numpy as jnp
import ml_dtypes
import numpy as np
from jax import lax
from jax.experimental import pallas as pl
from jax.experimental.pallas import tpu as pltpu
from jax.sharding import PartitionSpec as P

HALO = 128
BAND = 128
ITERS = 2

LEVEL = 0.4
SLOPE_FLOOR = 0.05
SHARPNESS = 8.0
CHUNK = 256
ROWS = 32
UNROLL = 4
OPERANDS = 19
VMEM_LIMIT = 32 * 1024 * 1024
MESH = pl.DeviceIdType.MESH
F32 = jnp.float32
BF16 = jnp.bfloat16


def pieces_of(table):
    high = table.astype(ml_dtypes.bfloat16)
    rest = table - high.astype(np.float64)
    middle = rest.astype(ml_dtypes.bfloat16)
    low = (rest - middle.astype(np.float64)).astype(ml_dtypes.bfloat16)
    return high, middle, low


def tables(tile):
    ext = tile + 2 * HALO
    half = BAND // 2
    step = 2.0 * math.pi / ext
    rows = -(-(2 * half + 1) // 16) * 16
    span = np.arange(ext) - (ext - 1) / 2
    positive = np.arange(half + 1)
    freq = np.arange(BAND) - half
    forward = np.zeros((rows, ext))
    forward[: half + 1] = np.cos(step * positive[:, None] * span[None])
    forward[half + 1 : 2 * half + 1] = np.sin(step * positive[1:, None] * span[None])
    pairs = np.arange(half)
    phase = step * span[:, None] * np.concatenate([pairs, -1 - pairs])[None]
    across = np.concatenate([np.cos(phase), np.sin(phase)], axis=1)
    across = np.concatenate([across[HALO:-HALO], across[:HALO], across[-HALO:]], axis=0)
    expand = np.zeros((2 * BAND, 2 * BAND))
    for place, number in enumerate(freq):
        expand[place, abs(number)] = 1.0
        if number != 0:
            expand[BAND + place, half + abs(number)] = np.sign(number)
    pixels = np.arange(tile // 2) + 0.5
    angle = step * pixels[:, None] * (freq[None] + 0.5)
    back_rows = np.concatenate([np.cos(angle), np.sin(angle)], axis=0) / ext
    angle = step * (pairs[:, None] + 0.5) * pixels[None]
    turn = np.eye(half)[::-1]
    turn = np.block([[turn, 0 * turn], [0 * turn, turn]]).astype(ml_dtypes.bfloat16)
    flip = np.eye(tile // 2)[::-1].astype(ml_dtypes.bfloat16)
    high, middle, low = pieces_of(back_rows)
    rows6 = np.concatenate([high, high, middle, high, middle, low], axis=1)
    cols6 = []
    for wave in (np.cos(angle), np.sin(angle)):
        high, middle, low = pieces_of(wave / ext)
        none = np.zeros_like(high)
        cols6.append(np.concatenate([high, high, high, low], axis=0))
        cols6.append(np.concatenate([middle, middle, none, none], axis=0))
    cols6 = np.concatenate(
        [np.concatenate(cols6[:2], axis=1), np.concatenate(cols6[2:], axis=1)], axis=0
    )
    return (
        np.concatenate(pieces_of(forward), axis=0),
        np.concatenate(pieces_of(across), axis=0),
        np.concatenate([expand] * 3, axis=1).astype(ml_dtypes.bfloat16),
        rows6,
        cols6,
        np.concatenate([flip] * 3, axis=1),
        np.concatenate([flip] * 3, axis=0),
        np.concatenate([turn] * 3, axis=0),
    )


def split(value):
    high = value.astype(BF16)
    low = (value - high.astype(F32)).astype(BF16)
    return high, low


def split3(value):
    high = value.astype(BF16)
    rest = value - high.astype(F32)
    middle = rest.astype(BF16)
    low = (rest - middle.astype(F32)).astype(BF16)
    return high, middle, low


def dot(left, right):
    return jnp.dot(left, right, preferred_element_type=F32)


def strip_sum(row_start, col_start, frag_len, orient, shift, extent):
    lower = jnp.minimum(shift, 0)
    upper = jnp.maximum(shift, 0)
    along = orient == 0
    row_low = jnp.where(along, row_start, row_start + lower)
    row_high = jnp.where(along, row_start + frag_len, row_start + upper)
    col_low = jnp.where(along, col_start + lower, col_start)
    col_high = jnp.where(along, col_start + upper, col_start + frag_len)
    position = lax.broadcasted_iota(jnp.int32, (extent, shift.shape[1]), 0)
    signs = jnp.where(shift > 0, 1.0, jnp.where(shift < 0, -1.0, 0.0))
    row_select = jnp.where((position >= row_low) & (position < row_high), signs, 0.0).astype(BF16)
    col_select = jnp.where((position >= col_low) & (position < col_high), 1.0, 0.0).astype(BF16)
    return lax.dot_general(
        row_select, col_select, (((1,), (1,)), ((), ())), preferred_element_type=F32
    )


def kernel(sizes, *refs):
    away, outs = refs[:OPERANDS], refs[OPERANDS : OPERANDS + 4]
    here, rest = refs[OPERANDS + 4 : 2 * OPERANDS + 4], refs[2 * OPERANDS + 4 :]
    sems = rest[-1]
    copies = [
        pltpu.make_async_copy(src, dst, sems.at[i]) for i, (src, dst) in enumerate(zip(away, here))
    ]

    def need(*numbers):
        for number in numbers:
            copies[number].wait()

    def start(*numbers):
        for number in numbers:
            copies[number].start()

    body(sizes, start, need, *here, *outs, *rest[:-1])


def body(
    sizes,
    begin,
    need,
    mask_ref,
    frow_ref,
    fcol_ref,
    flen_ref,
    fori_ref,
    fmove_ref,
    srow_ref,
    scol_ref,
    spec_ref,
    weight_ref,
    tol_ref,
    forward_ref,
    across_ref,
    expand_ref,
    rows_ref,
    cols_ref,
    flip_wide_ref,
    flip_tall_ref,
    turn_ref,
    intensity_ref,
    mask_out_ref,
    errors_ref,
    stats_ref,
    ext,
    hext,
    paired,
    stacked_a,
    stacked_b,
    sbuf,
    folded,
    choose,
    img,
    img_rx,
    err,
    err_rx,
    stat,
    stat_rx,
    halo_send,
    halo_recv,
    ka_send,
    ka_recv,
    stat_send,
    stat_recv,
    token,
):
    n_tx, n_ty, n_ka = sizes
    count = n_tx * n_ty * n_ka
    tile = mask_ref.shape[0]
    wide = ext.shape[1]
    sites = srow_ref.shape[2]
    kernels = spec_ref.shape[0]
    group = lax.axis_index("groups")
    tx = lax.axis_index("tx")
    ty = lax.axis_index("ty")
    ka = lax.axis_index("ka")
    me = (tx * n_ty + ty) * n_ka + ka

    def place(number):
        return (
            group,
            lax.div(number, n_ty * n_ka),
            lax.rem(lax.div(number, n_ka), n_ty),
            lax.rem(number, n_ka),
        )

    def remote(src, dst, send, recv, target):
        return pltpu.make_async_remote_copy(
            src_ref=src, dst_ref=dst, send_sem=send, recv_sem=recv, device_id=target, device_id_type=MESH
        )

    begin(1, 2, 3, 4, 5, 0, 9, 7, 18, 8, 11, 12, 13, 14, 15, 6, 10, 16, 17)
    barrier = pltpu.get_barrier_semaphore()

    partner = (group, tx, ty, 1 - ka)
    up = (group, tx - 1, ty, ka)
    down = (group, tx + 1, ty, ka)
    left = (group, tx, ty - 1, ka)
    right = (group, tx, ty + 1, ka)
    around = ((tx > 0, up), (tx < n_tx - 1, down), (ty > 0, left), (ty < n_ty - 1, right))

    def signal(semaphore, target):
        pl.semaphore_signal(semaphore, inc=1, device_id=target, device_id_type=MESH)

    signal(barrier, partner)
    for there, target in around:
        pl.when(there)(functools.partial(signal, barrier, target))

    need(1, 2, 3, 4, 5, 0)
    fragments = (frow_ref[0], fcol_ref[0], flen_ref[0], fori_ref[0])
    early = lax.div(n_ty - 1 - ty, max(n_ty - 1, 1))
    halves = (early, 1 - early)

    def to_up(half):
        return remote(
            ext.at[half, pl.ds(HALO, HALO)],
            ext.at[half, pl.ds(HALO + tile, HALO)],
            halo_send.at[half],
            halo_recv.at[half],
            up,
        )

    def to_down(half):
        return remote(
            ext.at[half, pl.ds(tile, HALO)],
            ext.at[half, pl.ds(0, HALO)],
            halo_send.at[2 + half],
            halo_recv.at[2 + half],
            down,
        )

    def chain(hop, at, count_at, before, after, previous, following):
        if 0 < hop:
            pl.when(at == hop)(lambda: pl.semaphore_wait(token.at[before], 1))
            pl.when(at == count_at - 1 - hop)(lambda: pl.semaphore_wait(token.at[after], 1))
        if hop < count_at - 1:
            pl.when(at == hop)(lambda: signal(token.at[before], following))
            pl.when(at == count_at - 1 - hop)(lambda: signal(token.at[after], previous))

    def pass_across(hop):
        chain(hop, ty, n_ty, 0, 1, left, right)

    def pass_on(hop):
        chain(hop, tx, n_tx, 2, 3, up, down)

    def send_rows():
        for half in halves:
            pl.when(tx > 0)(lambda: to_up(half).start())
            pl.when(tx < n_tx - 1)(lambda: to_down(half).start())

    def place_rows(values):
        for half in range(2):
            ext[half, HALO : HALO + tile, :] = values[:, half * HALO : (half + 1) * HALO]

    peers = 1
    for at, count_at in ((tx, n_tx), (ty, n_ty)):
        for steps in (at, count_at - 1 - at):
            peers = peers + lax.div(steps + count_at - 1, count_at)

    def send_off():
        pl.semaphore_wait(barrier, peers)
        send_rows()
        pass_across(0)

    first = jnp.clip(mask_ref[...] + strip_sum(*fragments, fmove_ref[0, 0, 0:1, :], tile), 0.0, 1.0)
    place_rows(first)
    second = jnp.clip(first + strip_sum(*fragments, fmove_ref[0, 0, 1:2, :], tile), 0.0, 1.0)
    mask_out_ref[...] = second
    pl.when(ka == 1)(lambda: place_rows(second))
    send_off()

    def fold(at):
        return jnp.where(at < tile // 2, tile - 1 - at, at - tile // 2)

    need(7)
    position = lax.broadcasted_iota(jnp.int32, (tile, CHUNK), 0)
    for start in range(0, sites, CHUNK):
        at_cols = fold(scol_ref[0, :, start : start + CHUNK])
        choose[:, start : start + CHUNK] = jnp.where(position == at_cols, 1.0, 0.0).astype(BF16)

    lower_lanes = lax.broadcasted_iota(jnp.int32, (BAND, BAND), 1) < BAND // 2

    def swap(value):
        return pltpu.roll(value, BAND // 2, 1)

    def pair(k):
        scale = jnp.sqrt(jnp.full((1, BAND), weight_ref[k], F32))
        k_re, k_im = spec_ref[k, 0], spec_ref[k, 1]
        below = jnp.where(lower_lanes, k_re, swap(k_im)) * scale
        paired[k, 0] = jnp.where(lower_lanes, swap(k_re), k_im) * scale
        paired[k, 1] = dot(jnp.concatenate(split3(below), axis=1), turn_ref[...])

    def pair_step(k, carry):
        for number in range(4):
            pair(4 * k + number)
        return carry

    need(9, 8, 18)
    lax.fori_loop(0, kernels // 4, pair_step, 0)
    for k in range(kernels // 4 * 4, kernels):
        pair(k)

    @pl.when(tx == 0)
    def _():
        ext[:, 0:HALO, :] = jnp.zeros((2, HALO, HALO), F32)

    @pl.when(tx == n_tx - 1)
    def _():
        ext[:, HALO + tile : wide, :] = jnp.zeros((2, HALO, HALO), F32)

    @pl.when(ty == 0)
    def _():
        hext[0] = jnp.zeros(hext.shape[1:], F32)

    @pl.when(ty == n_ty - 1)
    def _():
        hext[3] = jnp.zeros(hext.shape[1:], F32)

    rows = hext.shape[1]
    need(11)
    to_left = remote(hext.at[1], hext.at[3], halo_send.at[4], halo_recv.at[4], left)
    to_right = remote(hext.at[2], hext.at[0], halo_send.at[5], halo_recv.at[5], right)
    for half in halves:
        pl.when(tx > 0)(lambda: to_down(half).wait_recv())
        pl.when(tx < n_tx - 1)(lambda: to_up(half).wait_recv())
        high, middle, low = split3(ext[half])
        by = dot(forward_ref[...], jnp.concatenate([high, middle], axis=1))
        by_high, by_middle = by[:, :HALO], by[:, HALO:]
        by_low = dot(forward_ref[0:rows, :], low)
        total = (by_low + by_high[2 * rows :] + by_middle[rows : 2 * rows]) + (
            by_high[rows : 2 * rows] + by_middle[:rows]
        )
        hext[1 + half] = total + by_high[:rows]
        pl.when((half == 0) & (ty > 0))(to_left.start)
        pl.when((half == 1) & (ty < n_ty - 1))(to_right.start)

    for hop in range(1, n_ty):
        pass_across(hop)
    to_spec = remote(
        paired.at[pl.ds(0, kernels)],
        paired.at[pl.ds(kernels, kernels)],
        ka_send.at[0],
        ka_recv.at[0],
        partner,
    )
    to_spec.start()
    pass_on(0)
    need(12, 13)

    def column_part(block, first_row):
        high, middle, low = split3(block)
        depth = block.shape[1]

        def piece(number):
            return across_ref[number * wide + first_row : number * wide + first_row + depth, :]

        by_high = dot(jnp.concatenate([high, middle, low], axis=0), piece(0))
        by_middle = dot(jnp.concatenate([high, middle], axis=0), piece(1))
        by_low = dot(high, piece(2))
        part = (by_low + by_high[2 * rows :] + by_middle[rows:]) + (
            by_high[rows : 2 * rows] + by_middle[:rows]
        )
        return part + by_high[:rows]

    own_part = column_part(jnp.concatenate([hext[1], hext[2]], axis=1), 0)

    @pl.when(ty > 0)
    def _():
        to_right.wait_recv()

    @pl.when(ty < n_ty - 1)
    def _():
        to_left.wait_recv()

    pass_on(1)
    full = own_part + column_part(jnp.concatenate([hext[0], hext[3]], axis=1), tile)
    full = jnp.concatenate([full, jnp.zeros((2 * BAND - rows, 2 * BAND), F32)], axis=0)
    mixed = dot(expand_ref[...], jnp.concatenate(split3(full), axis=0))
    s_re = mixed[:BAND, :BAND] - mixed[BAND:, BAND:]
    s_im = -(mixed[BAND:, :BAND] + mixed[:BAND, BAND:])
    sbuf[0] = jnp.where(lower_lanes, s_re, swap(s_re))
    sbuf[1] = jnp.where(lower_lanes, -s_im, swap(s_im))
    sbuf[2] = jnp.where(lower_lanes, swap(s_re), s_re)
    sbuf[3] = jnp.where(lower_lanes, -swap(s_im), s_im)

    mid = tile // 2
    folded[0] = jnp.zeros(folded.shape[1:], F32)

    to_sbuf = remote(
        sbuf.at[pl.ds(0, 4)], sbuf.at[pl.ds(4, 4)], ka_send.at[1], ka_recv.at[1], partner
    )
    pl.when(ka == 0)(to_sbuf.start)
    to_share = remote(folded.at[1], folded.at[1], ka_send.at[4], ka_recv.at[4], partner)

    low_half = lax.broadcasted_iota(jnp.int32, (tile, BAND), 1) < BAND // 2

    def first_stage(k, stacked, slot=0):
        first = 4 * slot
        plus, minus = paired[k, 0], paired[k, 1]
        p_plus = plus * sbuf[first] + swap(plus) * sbuf[first + 1]
        p_minus = minus * sbuf[first + 2] + swap(minus) * sbuf[first + 3]
        high, middle, low = split3(
            jnp.concatenate([p_plus + p_minus, p_plus - p_minus], axis=1)
        )
        inner = dot(
            rows_ref[...], jnp.concatenate([high, middle, high, low, middle, high], axis=0)
        )
        for number in range(2):
            part = inner[:, number * BAND : (number + 1) * BAND]
            high, middle, low = split3(part)
            high_turned, middle_turned, low_turned = swap(high), swap(middle), swap(low)
            blocks = (
                (jnp.where(low_half, high, middle_turned), jnp.where(low_half, low, high_turned)),
                (jnp.where(low_half, high_turned, middle), jnp.where(low_half, low_turned, high)),
            )
            for row in range(0, mid, ROWS):
                for place_in, (left_part, right_part) in enumerate(blocks):
                    for wave in range(2):
                        at = 4 * row + (2 * place_in + wave) * ROWS
                        taken = slice(wave * mid + row, wave * mid + row + ROWS)
                        stacked[number, at : at + ROWS, :BAND] = left_part[taken]
                        stacked[number, at : at + ROWS, BAND:] = right_part[taken]

    def across_part(stacked, number, row):
        turned = dot(
            stacked[number, 4 * row : 4 * (row + ROWS), :],
            cols_ref[number * tile : (number + 1) * tile, :],
        )
        whole = turned[:, :mid] + turned[:, mid:]
        return [whole[quarter * ROWS : (quarter + 1) * ROWS] for quarter in range(4)]

    def second_stage(stacked, slot=0):
        for row in range(0, mid, ROWS):
            cc_re, sc_re, cc_im, sc_im = across_part(stacked, 0, row)
            cs_re, ss_re, cs_im, ss_im = across_part(stacked, 1, row)

            def both(side, x_re, x_im, y_re, y_im):
                at = (slot, slice(row, row + ROWS), slice(side, side + mid))
                folded[at] += (x_re - y_im) * (x_re - y_im) + (x_im + y_re) * (x_im + y_re)
                at = (slot, slice(mid + row, mid + row + ROWS), slice(mid - side, tile - side))
                folded[at] += (x_re + y_im) * (x_re + y_im) + (x_im - y_re) * (x_im - y_re)

            both(0, cc_re - ss_re, cc_im - ss_im, sc_re + cs_re, sc_im + cs_im)
            both(mid, cc_re + ss_re, cc_im + ss_im, sc_re - cs_re, sc_im - cs_im)

    stacks = (stacked_a, stacked_b)
    shared = 2 * kernels - UNROLL
    assert shared % UNROLL == 0 and kernels >= UNROLL

    def some_kernels(k, carry):
        for number in range(UNROLL):
            following = jnp.minimum(UNROLL * k + number + 1, shared - 1)
            first_stage(following, stacks[(number + 1) % 2])
            second_stage(stacks[number % 2])
        return carry

    def last_kernels(part, carry):
        first, slot = kernels - UNROLL + kernels * part, 1 - part
        first_stage(first, stacks[0], slot)
        for number in range(UNROLL):
            if number < UNROLL - 1:
                first_stage(first + number + 1, stacks[(number + 1) % 2], slot)
            second_stage(stacks[number % 2], slot)
        pl.when(part == 0)(to_share.start)
        return carry

    need(14, 15)
    first_stage(0, stacked_a)
    half_way = (kernels - 1) // UNROLL
    lax.fori_loop(0, half_way, some_kernels, 0)
    pass_on(2)
    to_spec.wait_recv()
    lax.fori_loop(half_way, shared // UNROLL, some_kernels, 0)

    @pl.when(ka == 1)
    def _():
        folded[1] = jnp.zeros(folded.shape[1:], F32)
        to_sbuf.wait_recv()
        lax.fori_loop(0, 2, last_kernels, 0)

    @pl.when(ka == 0)
    def _():
        to_share.wait_recv()
        folded[0] += folded[1]

    for hop in range(3, n_tx):
        pass_on(hop)
    image = folded[0]

    def gradient(axis):
        along = lax.broadcasted_iota(jnp.int32, (tile, tile), axis)
        before = jnp.where(
            lax.rem(along, mid) == 0, pltpu.roll(image, mid, axis), pltpu.roll(image, 1, axis)
        )
        return (pltpu.roll(image, tile - 1, axis) - before) * 0.5

    grad_rows, grad_cols = gradient(0), gradient(1)
    slope = jnp.sqrt(grad_rows * grad_rows + grad_cols * grad_cols)
    error_map = (image - LEVEL) / jnp.maximum(slope, SLOPE_FLOOR)
    high, low = split(error_map)
    need(6, 10)
    limit = tol_ref[ka].astype(F32) / 8.0
    peak = jnp.zeros((1, CHUNK), F32)
    total = jnp.zeros((1, CHUNK), F32)
    for start in range(0, sites, CHUNK):
        at_rows = fold(srow_ref[0, :, start : start + CHUNK])
        picked = dot(high, choose[:, start : start + CHUNK]) + dot(low, choose[:, start : start + CHUNK])
        errors = jnp.sum(jnp.where(position == at_rows, picked, 0.0), axis=0, keepdims=True)
        err[:, start : start + CHUNK] = errors
        size = jnp.abs(errors)
        peak = jnp.maximum(peak, size)
        total = total + 1.0 / (1.0 + jnp.exp(-SHARPNESS * (limit - size)))
    stat[0:1, :] = functools.reduce(
        jnp.maximum, [peak[:, i : i + 128] for i in range(0, CHUNK, 128)]
    )
    stat[1:2, :] = functools.reduce(
        jnp.add, [total[:, i : i + 128] for i in range(0, CHUNK, 128)]
    )
    to_err = remote(err, err_rx, ka_send.at[3], ka_recv.at[3], partner)
    to_err.start()

    def to_stat(offset):
        return remote(
            stat,
            stat_rx.at[me],
            stat_send.at[offset],
            stat_recv.at[me],
            place(lax.rem(me + offset, count)),
        )

    def send_stat(offset, carry):
        to_stat(offset).start()
        return carry

    lax.fori_loop(1, count, send_stat, 0)
    stat_rx[pl.ds(me, 1)] = stat[...][None]

    to_img = remote(img, img_rx, ka_send.at[2], ka_recv.at[2], partner)
    need(16, 17)

    @pl.when(ka == ITERS - 1)
    def _():
        lower = jnp.concatenate(split3(folded[0, mid:, :]), axis=0)
        ordered = jnp.concatenate([dot(flip_wide_ref[...], lower), folded[0, :mid, :]], axis=0)
        lower = jnp.concatenate(split3(ordered[:, mid:]), axis=1)
        result = jnp.concatenate([dot(lower, flip_tall_ref[...]), ordered[:, :mid]], axis=1)
        img[...] = result
        to_img.start()
        intensity_ref[...] = result

    @pl.when(ka < ITERS - 1)
    def _():
        to_img.wait_recv()
        intensity_ref[...] = img_rx[...]

    to_err.wait_recv()
    mine = err[...]
    theirs = err_rx[...]
    errors_ref[0, 0, 0:1, :] = jnp.where(ka == 0, mine, theirs)
    errors_ref[0, 0, 1:2, :] = jnp.where(ka == 0, theirs, mine)

    def wait_stat(offset, carry):
        to_stat(offset).wait_send()
        source = lax.rem(me + offset, count)
        remote(
            stat, stat_rx.at[source], stat_send.at[offset], stat_recv.at[source], place(source)
        ).wait_recv()
        return carry

    lax.fori_loop(1, count, wait_stat, 0)

    for which in range(ITERS):
        rows_of = range(which, count, n_ka)
        stats_ref[which : which + 1, :] = functools.reduce(
            jnp.maximum, [stat_rx[number, 0:1, :] for number in rows_of]
        )
        stats_ref[ITERS + which : ITERS + which + 1, :] = functools.reduce(
            jnp.add, [stat_rx[number, 1:2, :] for number in rows_of]
        )

    for half in range(2):
        pl.when(tx > 0)(lambda: to_up(half).wait_send())
        pl.when(tx < n_tx - 1)(lambda: to_down(half).wait_send())

    @pl.when(ty > 0)
    def _():
        to_left.wait_send()

    @pl.when(ty < n_ty - 1)
    def _():
        to_right.wait_send()

    pl.when(ka == ITERS - 1)(to_img.wait_send)
    pl.when(ka == 0)(to_sbuf.wait_send)
    pl.when(ka == 1)(to_share.wait_send)
    for copy in (to_spec, to_err):
        copy.wait_send()


def write(scale, image, mask, errors, stats, image_out, mask_out, errors_out, peaks, shares, sems):
    copies = [
        pltpu.make_async_copy(src, dst, sems.at[i])
        for i, (src, dst) in enumerate(((image, image_out), (mask, mask_out), (errors, errors_out)))
    ]
    for copy in copies:
        copy.start()
    for i in range(ITERS):
        peaks[i] = jnp.max(stats[i : i + 1, :])
        shares[i] = jnp.sum(stats[ITERS + i : ITERS + i + 1, :]) * scale
    for copy in copies:
        copy.wait()


def shards(sizes, *args):
    mask_raster, spectra = args[0], args[8]
    site_count = args[6].shape[2]
    tile = mask_raster.shape[0]
    wide = tile + 2 * HALO
    consts = [jnp.asarray(a) for a in tables(tile)]
    rows = consts[0].shape[0] // 3
    kernels = spectra.shape[0]
    count = sizes[0] * sizes[1] * sizes[2]
    vmem = pl.BlockSpec(memory_space=pltpu.VMEM)
    smem = pl.BlockSpec(memory_space=pltpu.SMEM)
    dma = pltpu.SemaphoreType.DMA
    operands = tuple(
        pltpu.with_memory_space_constraint(a, pltpu.HBM) for a in (*args, *consts)
    )
    local = [
        (pltpu.SMEM if number in (9, 10) else pltpu.VMEM)(a.shape, a.dtype)
        for number, a in enumerate(operands)
    ]
    tile_shape = (tile, tile)
    error_shape = (1, 1, ITERS, site_count)
    results = pl.pallas_call(
            functools.partial(kernel, sizes),
            out_shape=(
                pltpu.VMEM(tile_shape, F32),
                pltpu.VMEM(tile_shape, F32),
                pltpu.VMEM(error_shape, F32),
                pltpu.VMEM((8, 128), F32),
            ),
            in_specs=[pl.BlockSpec(memory_space=pltpu.HBM)] * OPERANDS,
            out_specs=(vmem,) * 4,
            scratch_shapes=local
            + [
                pltpu.VMEM((2, wide, HALO), F32),
                pltpu.VMEM((4, rows, HALO), F32),
                pltpu.VMEM((2 * kernels, *spectra.shape[1:]), F32),
                pltpu.VMEM((2, 2 * tile, tile), BF16),
                pltpu.VMEM((2, 2 * tile, tile), BF16),
                pltpu.VMEM((8, BAND, BAND), F32),
                pltpu.VMEM((2, tile, tile), F32),
                pltpu.VMEM((tile, site_count), BF16),
                pltpu.VMEM((tile, tile), F32),
                pltpu.VMEM((tile, tile), F32),
                pltpu.VMEM((1, site_count), F32),
                pltpu.VMEM((1, site_count), F32),
                pltpu.VMEM((2, 128), F32),
                pltpu.VMEM((count, 2, 128), F32),
                dma((6,)),
                dma((6,)),
                dma((5,)),
                dma((5,)),
                dma((count,)),
                dma((count,)),
                pltpu.SemaphoreType.REGULAR((4,)),
                dma((OPERANDS,)),
            ],
            compiler_params=pltpu.CompilerParams(
                collective_id=0, has_side_effects=True, vmem_limit_bytes=VMEM_LIMIT
            ),
        )(*operands)
    hbm = pl.BlockSpec(memory_space=pltpu.HBM)
    return tuple(
        pl.pallas_call(
            functools.partial(write, 1.0 / (site_count * sizes[0] * sizes[1])),
            out_shape=(
                jax.ShapeDtypeStruct(tile_shape, F32),
                jax.ShapeDtypeStruct(tile_shape, F32),
                jax.ShapeDtypeStruct(error_shape, F32),
                jax.ShapeDtypeStruct((ITERS,), F32),
                jax.ShapeDtypeStruct((ITERS,), F32),
            ),
            in_specs=[vmem] * 4,
            out_specs=(hbm, hbm, hbm, smem, smem),
            scratch_shapes=[dma((3,))],
            compiler_params=pltpu.CompilerParams(vmem_limit_bytes=VMEM_LIMIT),
        )(*results)
    )


def solution(mesh):
    sizes = tuple(mesh.shape[axis] for axis in ("tx", "ty", "ka"))
    assert sizes[2] == ITERS
    placed = (
        P(("groups", "tx"), "ty"),
        P(("groups", "tx"), "ty", None),
        P(("groups", "tx"), "ty", None),
        P(("groups", "tx"), "ty", None),
        P(("groups", "tx"), "ty", None),
        P(("groups", "tx"), "ty", None, None),
        P(("groups", "tx"), "ty", None),
        P(("groups", "tx"), "ty", None),
        P("ka", None, None, None),
        P("ka"),
        P(),
    )
    return jax.shard_map(
        functools.partial(shards, sizes),
        mesh=mesh,
        in_specs=placed,
        out_specs=(
            P(("groups", "tx"), "ty"),
            P(("groups", "tx"), "ty"),
            P(("groups", "tx"), "ty", None, None),
            P("groups"),
            P("groups"),
        ),
        check_vma=False,
    )
```

```python
import functools
import math

import jax
import jax.numpy as jnp
import ml_dtypes
import numpy as np
from jax import lax
from jax.experimental import pallas as pl
from jax.experimental.pallas import tpu as pltpu
from jax.sharding import PartitionSpec as P

HALO = 128
BAND = 128
ITERS = 2

LEVEL = 0.4
SLOPE_FLOOR = 0.05
SHARPNESS = 8.0
CHUNK = 256
ROWS = 32
UNROLL = 4
OPERANDS = 19
VMEM_LIMIT = 32 * 1024 * 1024
MESH = pl.DeviceIdType.MESH
F32 = jnp.float32
BF16 = jnp.bfloat16


def pieces_of(table):
    high = table.astype(ml_dtypes.bfloat16)
    rest = table - high.astype(np.float64)
    middle = rest.astype(ml_dtypes.bfloat16)
    low = (rest - middle.astype(np.float64)).astype(ml_dtypes.bfloat16)
    return high, middle, low


def tables(tile):
    ext = tile + 2 * HALO
    half = BAND // 2
    step = 2.0 * math.pi / ext
    rows = -(-(2 * half + 1) // 16) * 16
    span = np.arange(ext) - (ext - 1) / 2
    positive = np.arange(half + 1)
    freq = np.arange(BAND) - half
    forward = np.zeros((rows, ext))
    forward[: half + 1] = np.cos(step * positive[:, None] * span[None])
    forward[half + 1 : 2 * half + 1] = np.sin(step * positive[1:, None] * span[None])
    pairs = np.arange(half)
    phase = step * span[:, None] * np.concatenate([pairs, -1 - pairs])[None]
    across = np.concatenate([np.cos(phase), np.sin(phase)], axis=1)
    across = np.concatenate([across[HALO:-HALO], across[:HALO], across[-HALO:]], axis=0)
    expand = np.zeros((2 * BAND, 2 * BAND))
    for place, number in enumerate(freq):
        expand[place, abs(number)] = 1.0
        if number != 0:
            expand[BAND + place, half + abs(number)] = np.sign(number)
    pixels = np.arange(tile // 2) + 0.5
    angle = step * pixels[:, None] * (freq[None] + 0.5)
    back_rows = np.concatenate([np.cos(angle), np.sin(angle)], axis=0) / ext
    angle = step * (pairs[:, None] + 0.5) * pixels[None]
    turn = np.eye(half)[::-1]
    turn = np.block([[turn, 0 * turn], [0 * turn, turn]]).astype(ml_dtypes.bfloat16)
    flip = np.eye(tile // 2)[::-1].astype(ml_dtypes.bfloat16)
    high, middle, low = pieces_of(back_rows)
    rows6 = np.concatenate([high, high, middle, high, middle, low], axis=1)
    cols6 = []
    for wave in (np.cos(angle), np.sin(angle)):
        high, middle, low = pieces_of(wave / ext)
        none = np.zeros_like(high)
        cols6.append(np.concatenate([high, high, high, low], axis=0))
        cols6.append(np.concatenate([middle, middle, none, none], axis=0))
    cols6 = np.concatenate(
        [np.concatenate(cols6[:2], axis=1), np.concatenate(cols6[2:], axis=1)], axis=0
    )
    return (
        np.concatenate(pieces_of(forward), axis=0),
        np.concatenate(pieces_of(across), axis=0),
        np.concatenate([expand] * 3, axis=1).astype(ml_dtypes.bfloat16),
        rows6,
        cols6,
        np.concatenate([flip] * 3, axis=1),
        np.concatenate([flip] * 3, axis=0),
        np.concatenate([turn] * 3, axis=0),
    )


def split(value):
    high = value.astype(BF16)
    low = (value - high.astype(F32)).astype(BF16)
    return high, low


def split3(value):
    high = value.astype(BF16)
    rest = value - high.astype(F32)
    middle = rest.astype(BF16)
    low = (rest - middle.astype(F32)).astype(BF16)
    return high, middle, low


def dot(left, right):
    return jnp.dot(left, right, preferred_element_type=F32)


def strip_sum(row_start, col_start, frag_len, orient, shift, extent):
    lower = jnp.minimum(shift, 0)
    upper = jnp.maximum(shift, 0)
    along = orient == 0
    row_low = jnp.where(along, row_start, row_start + lower)
    row_high = jnp.where(along, row_start + frag_len, row_start + upper)
    col_low = jnp.where(along, col_start + lower, col_start)
    col_high = jnp.where(along, col_start + upper, col_start + frag_len)
    position = lax.broadcasted_iota(jnp.int32, (extent, shift.shape[1]), 0)
    signs = jnp.where(shift > 0, 1.0, jnp.where(shift < 0, -1.0, 0.0))
    row_select = jnp.where((position >= row_low) & (position < row_high), signs, 0.0).astype(BF16)
    col_select = jnp.where((position >= col_low) & (position < col_high), 1.0, 0.0).astype(BF16)
    return lax.dot_general(
        row_select, col_select, (((1,), (1,)), ((), ())), preferred_element_type=F32
    )


def kernel(sizes, *refs):
    away, outs = refs[:OPERANDS], refs[OPERANDS : OPERANDS + 4]
    here, rest = refs[OPERANDS + 4 : 2 * OPERANDS + 4], refs[2 * OPERANDS + 4 :]
    sems = rest[-1]
    copies = [
        pltpu.make_async_copy(src, dst, sems.at[i]) for i, (src, dst) in enumerate(zip(away, here))
    ]

    def need(*numbers):
        for number in numbers:
            copies[number].wait()

    def start(*numbers):
        for number in numbers:
            copies[number].start()

    body(sizes, start, need, *here, *outs, *rest[:-1])


def body(
    sizes,
    begin,
    need,
    mask_ref,
    frow_ref,
    fcol_ref,
    flen_ref,
    fori_ref,
    fmove_ref,
    srow_ref,
    scol_ref,
    spec_ref,
    weight_ref,
    tol_ref,
    forward_ref,
    across_ref,
    expand_ref,
    rows_ref,
    cols_ref,
    flip_wide_ref,
    flip_tall_ref,
    turn_ref,
    intensity_ref,
    mask_out_ref,
    errors_ref,
    stats_ref,
    ext,
    hext,
    paired,
    stacked_a,
    stacked_b,
    sbuf,
    folded,
    choose,
    img,
    img_rx,
    err,
    err_rx,
    stat,
    stat_rx,
    halo_send,
    halo_recv,
    ka_send,
    ka_recv,
    stat_send,
    stat_recv,
    token,
):
    n_tx, n_ty, n_ka = sizes
    count = n_tx * n_ty * n_ka
    tile = mask_ref.shape[0]
    wide = ext.shape[1]
    sites = srow_ref.shape[2]
    kernels = spec_ref.shape[0]
    group = lax.axis_index("groups")
    tx = lax.axis_index("tx")
    ty = lax.axis_index("ty")
    ka = lax.axis_index("ka")
    me = (tx * n_ty + ty) * n_ka + ka

    def place(number):
        return (
            group,
            lax.div(number, n_ty * n_ka),
            lax.rem(lax.div(number, n_ka), n_ty),
            lax.rem(number, n_ka),
        )

    def remote(src, dst, send, recv, target):
        return pltpu.make_async_remote_copy(
            src_ref=src, dst_ref=dst, send_sem=send, recv_sem=recv, device_id=target, device_id_type=MESH
        )

    begin(1, 2, 3, 4, 5, 0, 9, 7, 18, 8, 11, 12, 13, 14, 15, 6, 10, 16, 17)
    barrier = pltpu.get_barrier_semaphore()

    partner = (group, tx, ty, 1 - ka)
    up = (group, tx - 1, ty, ka)
    down = (group, tx + 1, ty, ka)
    left = (group, tx, ty - 1, ka)
    right = (group, tx, ty + 1, ka)
    around = ((tx > 0, up), (tx < n_tx - 1, down), (ty > 0, left), (ty < n_ty - 1, right))

    def signal(semaphore, target):
        pl.semaphore_signal(semaphore, inc=1, device_id=target, device_id_type=MESH)

    signal(barrier, partner)
    for there, target in around:
        pl.when(there)(functools.partial(signal, barrier, target))

    need(1, 2, 3, 4, 5, 0)
    fragments = (frow_ref[0], fcol_ref[0], flen_ref[0], fori_ref[0])
    early = lax.div(n_ty - 1 - ty, max(n_ty - 1, 1))
    halves = (early, 1 - early)

    def to_up(half):
        return remote(
            ext.at[half, pl.ds(HALO, HALO)],
            ext.at[half, pl.ds(HALO + tile, HALO)],
            halo_send.at[half],
            halo_recv.at[half],
            up,
        )

    def to_down(half):
        return remote(
            ext.at[half, pl.ds(tile, HALO)],
            ext.at[half, pl.ds(0, HALO)],
            halo_send.at[2 + half],
            halo_recv.at[2 + half],
            down,
        )

    def chain(hop, at, count_at, before, after, previous, following):
        if 0 < hop:
            pl.when(at == hop)(lambda: pl.semaphore_wait(token.at[before], 1))
            pl.when(at == count_at - 1 - hop)(lambda: pl.semaphore_wait(token.at[after], 1))
        if hop < count_at - 1:
            pl.when(at == hop)(lambda: signal(token.at[before], following))
            pl.when(at == count_at - 1 - hop)(lambda: signal(token.at[after], previous))

    def pass_across(hop):
        chain(hop, ty, n_ty, 0, 1, left, right)

    def pass_on(hop):
        chain(hop, tx, n_tx, 2, 3, up, down)

    def send_rows():
        for half in halves:
            pl.when(tx > 0)(lambda: to_up(half).start())
            pl.when(tx < n_tx - 1)(lambda: to_down(half).start())

    def place_rows(values):
        for half in range(2):
            ext[half, HALO : HALO + tile, :] = values[:, half * HALO : (half + 1) * HALO]

    peers = 1
    for at, count_at in ((tx, n_tx), (ty, n_ty)):
        for steps in (at, count_at - 1 - at):
            peers = peers + lax.div(steps + count_at - 1, count_at)

    def send_off():
        pl.semaphore_wait(barrier, peers)
        send_rows()
        pass_across(0)

    first = jnp.clip(mask_ref[...] + strip_sum(*fragments, fmove_ref[0, 0, 0:1, :], tile), 0.0, 1.0)
    place_rows(first)
    second = jnp.clip(first + strip_sum(*fragments, fmove_ref[0, 0, 1:2, :], tile), 0.0, 1.0)
    mask_out_ref[...] = second
    pl.when(ka == 1)(lambda: place_rows(second))
    send_off()

    def fold(at):
        return jnp.where(at < tile // 2, tile - 1 - at, at - tile // 2)

    need(7)
    position = lax.broadcasted_iota(jnp.int32, (tile, CHUNK), 0)
    for start in range(0, sites, CHUNK):
        at_cols = fold(scol_ref[0, :, start : start + CHUNK])
        choose[:, start : start + CHUNK] = jnp.where(position == at_cols, 1.0, 0.0).astype(BF16)

    lower_lanes = lax.broadcasted_iota(jnp.int32, (BAND, BAND), 1) < BAND // 2

    def swap(value):
        return pltpu.roll(value, BAND // 2, 1)

    def pair(k):
        scale = jnp.sqrt(jnp.full((1, BAND), weight_ref[k], F32))
        k_re, k_im = spec_ref[k, 0], spec_ref[k, 1]
        below = jnp.where(lower_lanes, k_re, swap(k_im)) * scale
        paired[k, 0] = jnp.where(lower_lanes, swap(k_re), k_im) * scale
        paired[k, 1] = dot(jnp.concatenate(split3(below), axis=1), turn_ref[...])

    def pair_step(k, carry):
        for number in range(4):
            pair(4 * k + number)
        return carry

    need(9, 8, 18)
    lax.fori_loop(0, kernels // 4, pair_step, 0)
    for k in range(kernels // 4 * 4, kernels):
        pair(k)

    @pl.when(tx == 0)
    def _():
        ext[:, 0:HALO, :] = jnp.zeros((2, HALO, HALO), F32)

    @pl.when(tx == n_tx - 1)
    def _():
        ext[:, HALO + tile : wide, :] = jnp.zeros((2, HALO, HALO), F32)

    @pl.when(ty == 0)
    def _():
        hext[0] = jnp.zeros(hext.shape[1:], F32)

    @pl.when(ty == n_ty - 1)
    def _():
        hext[3] = jnp.zeros(hext.shape[1:], F32)

    rows = hext.shape[1]
    need(11)
    to_left = remote(hext.at[1], hext.at[3], halo_send.at[4], halo_recv.at[4], left)
    to_right = remote(hext.at[2], hext.at[0], halo_send.at[5], halo_recv.at[5], right)
    for half in halves:
        pl.when(tx > 0)(lambda: to_down(half).wait_recv())
        pl.when(tx < n_tx - 1)(lambda: to_up(half).wait_recv())
        high, middle, low = split3(ext[half])
        by = dot(forward_ref[...], jnp.concatenate([high, middle], axis=1))
        by_high, by_middle = by[:, :HALO], by[:, HALO:]
        by_low = dot(forward_ref[0:rows, :], low)
        total = (by_low + by_high[2 * rows :] + by_middle[rows : 2 * rows]) + (
            by_high[rows : 2 * rows] + by_middle[:rows]
        )
        hext[1 + half] = total + by_high[:rows]
        pl.when((half == 0) & (ty > 0))(to_left.start)
        pl.when((half == 1) & (ty < n_ty - 1))(to_right.start)

    for hop in range(1, n_ty):
        pass_across(hop)
    to_spec = remote(
        paired.at[pl.ds(0, kernels)],
        paired.at[pl.ds(kernels, kernels)],
        ka_send.at[0],
        ka_recv.at[0],
        partner,
    )
    to_spec.start()
    pass_on(0)
    need(12, 13)

    def column_part(block, first_row):
        high, middle, low = split3(block)
        depth = block.shape[1]

        def piece(number):
            return across_ref[number * wide + first_row : number * wide + first_row + depth, :]

        by_high = dot(jnp.concatenate([high, middle, low], axis=0), piece(0))
        by_middle = dot(jnp.concatenate([high, middle], axis=0), piece(1))
        by_low = dot(high, piece(2))
        part = (by_low + by_high[2 * rows :] + by_middle[rows:]) + (
            by_high[rows : 2 * rows] + by_middle[:rows]
        )
        return part + by_high[:rows]

    own_part = column_part(jnp.concatenate([hext[1], hext[2]], axis=1), 0)

    @pl.when(ty > 0)
    def _():
        to_right.wait_recv()

    @pl.when(ty < n_ty - 1)
    def _():
        to_left.wait_recv()

    pass_on(1)
    full = own_part + column_part(jnp.concatenate([hext[0], hext[3]], axis=1), tile)
    full = jnp.concatenate([full, jnp.zeros((2 * BAND - rows, 2 * BAND), F32)], axis=0)
    mixed = dot(expand_ref[...], jnp.concatenate(split3(full), axis=0))
    s_re = mixed[:BAND, :BAND] - mixed[BAND:, BAND:]
    s_im = -(mixed[BAND:, :BAND] + mixed[:BAND, BAND:])
    sbuf[0] = jnp.where(lower_lanes, s_re, swap(s_re))
    sbuf[1] = jnp.where(lower_lanes, -s_im, swap(s_im))
    sbuf[2] = jnp.where(lower_lanes, swap(s_re), s_re)
    sbuf[3] = jnp.where(lower_lanes, -swap(s_im), s_im)

    mid = tile // 2
    folded[0] = jnp.zeros(folded.shape[1:], F32)

    to_sbuf = remote(
        sbuf.at[pl.ds(0, 4)], sbuf.at[pl.ds(4, 4)], ka_send.at[1], ka_recv.at[1], partner
    )
    pl.when(ka == 0)(to_sbuf.start)
    to_share = remote(folded.at[1], folded.at[1], ka_send.at[4], ka_recv.at[4], partner)

    low_half = lax.broadcasted_iota(jnp.int32, (tile, BAND), 1) < BAND // 2

    def first_stage(k, stacked, slot=0):
        first = 4 * slot
        plus, minus = paired[k, 0], paired[k, 1]
        p_plus = plus * sbuf[first] + swap(plus) * sbuf[first + 1]
        p_minus = minus * sbuf[first + 2] + swap(minus) * sbuf[first + 3]
        high, middle, low = split3(
            jnp.concatenate([p_plus + p_minus, p_plus - p_minus], axis=1)
        )
        inner = dot(
            rows_ref[...], jnp.concatenate([high, middle, high, low, middle, high], axis=0)
        )
        for number in range(2):
            part = inner[:, number * BAND : (number + 1) * BAND]
            high, middle, low = split3(part)
            high_turned, middle_turned, low_turned = swap(high), swap(middle), swap(low)
            blocks = (
                (jnp.where(low_half, high, middle_turned), jnp.where(low_half, low, high_turned)),
                (jnp.where(low_half, high_turned, middle), jnp.where(low_half, low_turned, high)),
            )
            for row in range(0, mid, ROWS):
                for place_in, (left_part, right_part) in enumerate(blocks):
                    for wave in range(2):
                        at = 4 * row + (2 * place_in + wave) * ROWS
                        taken = slice(wave * mid + row, wave * mid + row + ROWS)
                        stacked[number, at : at + ROWS, :BAND] = left_part[taken]
                        stacked[number, at : at + ROWS, BAND:] = right_part[taken]

    def across_part(stacked, number, row):
        turned = dot(
            stacked[number, 4 * row : 4 * (row + ROWS), :],
            cols_ref[number * tile : (number + 1) * tile, :],
        )
        whole = turned[:, :mid] + turned[:, mid:]
        return [whole[quarter * ROWS : (quarter + 1) * ROWS] for quarter in range(4)]

    def second_stage(stacked, slot=0):
        for row in range(0, mid, ROWS):
            cc_re, sc_re, cc_im, sc_im = across_part(stacked, 0, row)
            cs_re, ss_re, cs_im, ss_im = across_part(stacked, 1, row)

            def both(side, x_re, x_im, y_re, y_im):
                at = (slot, slice(row, row + ROWS), slice(side, side + mid))
                folded[at] += (x_re - y_im) * (x_re - y_im) + (x_im + y_re) * (x_im + y_re)
                at = (slot, slice(mid + row, mid + row + ROWS), slice(mid - side, tile - side))
                folded[at] += (x_re + y_im) * (x_re + y_im) + (x_im - y_re) * (x_im - y_re)

            both(0, cc_re - ss_re, cc_im - ss_im, sc_re + cs_re, sc_im + cs_im)
            both(mid, cc_re + ss_re, cc_im + ss_im, sc_re - cs_re, sc_im - cs_im)

    stacks = (stacked_a, stacked_b)
    shared = 2 * kernels - UNROLL
    assert shared % UNROLL == 0 and kernels >= UNROLL

    def some_kernels(k, carry):
        for number in range(UNROLL):
            following = jnp.minimum(UNROLL * k + number + 1, shared - 1)
            first_stage(following, stacks[(number + 1) % 2])
            second_stage(stacks[number % 2])
        return carry

    def last_kernels(part, carry):
        first, slot = kernels - UNROLL + kernels * part, 1 - part
        first_stage(first, stacks[0], slot)
        for number in range(UNROLL):
            if number < UNROLL - 1:
                first_stage(first + number + 1, stacks[(number + 1) % 2], slot)
            second_stage(stacks[number % 2], slot)
        pl.when(part == 0)(to_share.start)
        return carry

    need(14, 15)
    first_stage(0, stacked_a)
    half_way = (kernels - 1) // UNROLL
    lax.fori_loop(0, half_way, some_kernels, 0)
    pass_on(2)
    to_spec.wait_recv()
    lax.fori_loop(half_way, shared // UNROLL, some_kernels, 0)

    @pl.when(ka == 1)
    def _():
        folded[1] = jnp.zeros(folded.shape[1:], F32)
        to_sbuf.wait_recv()
        lax.fori_loop(0, 2, last_kernels, 0)

    @pl.when(ka == 0)
    def _():
        to_share.wait_recv()
        folded[0] += folded[1]

    for hop in range(3, n_tx):
        pass_on(hop)
    image = folded[0]

    def gradient(axis):
        along = lax.broadcasted_iota(jnp.int32, (tile, tile), axis)
        before = jnp.where(
            lax.rem(along, mid) == 0, pltpu.roll(image, mid, axis), pltpu.roll(image, 1, axis)
        )
        return (pltpu.roll(image, tile - 1, axis) - before) * 0.5

    grad_rows, grad_cols = gradient(0), gradient(1)
    slope = jnp.sqrt(grad_rows * grad_rows + grad_cols * grad_cols)
    error_map = (image - LEVEL) / jnp.maximum(slope, SLOPE_FLOOR)
    high, low = split(error_map)
    need(6, 10)
    limit = tol_ref[ka].astype(F32) / 8.0
    peak = jnp.zeros((1, CHUNK), F32)
    total = jnp.zeros((1, CHUNK), F32)
    for start in range(0, sites, CHUNK):
        at_rows = fold(srow_ref[0, :, start : start + CHUNK])
        picked = dot(high, choose[:, start : start + CHUNK]) + dot(low, choose[:, start : start + CHUNK])
        errors = jnp.sum(jnp.where(position == at_rows, picked, 0.0), axis=0, keepdims=True)
        err[:, start : start + CHUNK] = errors
        size = jnp.abs(errors)
        peak = jnp.maximum(peak, size)
        total = total + 1.0 / (1.0 + jnp.exp(-SHARPNESS * (limit - size)))
    stat[0:1, :] = functools.reduce(
        jnp.maximum, [peak[:, i : i + 128] for i in range(0, CHUNK, 128)]
    )
    stat[1:2, :] = functools.reduce(
        jnp.add, [total[:, i : i + 128] for i in range(0, CHUNK, 128)]
    )

    def to_stat(offset):
        return remote(
            stat,
            stat_rx.at[me],
            stat_send.at[offset],
            stat_recv.at[me],
            place(lax.rem(me + offset, count)),
        )

    for offset in sorted(range(1, count), key=lambda number: min(number, count - number)):
        to_stat(offset).start()
    to_err = remote(err, err_rx, ka_send.at[3], ka_recv.at[3], partner)
    to_err.start()
    stat_rx[pl.ds(me, 1)] = stat[...][None]

    to_img = remote(img, img_rx, ka_send.at[2], ka_recv.at[2], partner)
    need(16, 17)

    @pl.when(ka == ITERS - 1)
    def _():
        lower = jnp.concatenate(split3(folded[0, mid:, :]), axis=0)
        ordered = jnp.concatenate([dot(flip_wide_ref[...], lower), folded[0, :mid, :]], axis=0)
        lower = jnp.concatenate(split3(ordered[:, mid:]), axis=1)
        result = jnp.concatenate([dot(lower, flip_tall_ref[...]), ordered[:, :mid]], axis=1)
        img[...] = result
        to_img.start()
        intensity_ref[...] = result

    @pl.when(ka < ITERS - 1)
    def _():
        to_img.wait_recv()
        intensity_ref[...] = img_rx[...]

    to_err.wait_recv()
    mine = err[...]
    theirs = err_rx[...]
    errors_ref[0, 0, 0:1, :] = jnp.where(ka == 0, mine, theirs)
    errors_ref[0, 0, 1:2, :] = jnp.where(ka == 0, theirs, mine)

    def wait_stat(offset, carry):
        to_stat(offset).wait_send()
        source = lax.rem(me + offset, count)
        remote(
            stat, stat_rx.at[source], stat_send.at[offset], stat_recv.at[source], place(source)
        ).wait_recv()
        return carry

    lax.fori_loop(1, count, wait_stat, 0)

    for which in range(ITERS):
        rows_of = range(which, count, n_ka)
        stats_ref[which : which + 1, :] = functools.reduce(
            jnp.maximum, [stat_rx[number, 0:1, :] for number in rows_of]
        )
        stats_ref[ITERS + which : ITERS + which + 1, :] = functools.reduce(
            jnp.add, [stat_rx[number, 1:2, :] for number in rows_of]
        )

    for half in range(2):
        pl.when(tx > 0)(lambda: to_up(half).wait_send())
        pl.when(tx < n_tx - 1)(lambda: to_down(half).wait_send())

    @pl.when(ty > 0)
    def _():
        to_left.wait_send()

    @pl.when(ty < n_ty - 1)
    def _():
        to_right.wait_send()

    pl.when(ka == ITERS - 1)(to_img.wait_send)
    pl.when(ka == 0)(to_sbuf.wait_send)
    pl.when(ka == 1)(to_share.wait_send)
    for copy in (to_spec, to_err):
        copy.wait_send()


def write(scale, image, mask, errors, stats, image_out, mask_out, errors_out, peaks, shares, sems):
    copies = [
        pltpu.make_async_copy(src, dst, sems.at[i])
        for i, (src, dst) in enumerate(((image, image_out), (mask, mask_out), (errors, errors_out)))
    ]
    for copy in copies:
        copy.start()
    for i in range(ITERS):
        peaks[i] = jnp.max(stats[i : i + 1, :])
        shares[i] = jnp.sum(stats[ITERS + i : ITERS + i + 1, :]) * scale
    for copy in copies:
        copy.wait()


def shards(sizes, *args):
    mask_raster, spectra = args[0], args[8]
    site_count = args[6].shape[2]
    tile = mask_raster.shape[0]
    wide = tile + 2 * HALO
    consts = [jnp.asarray(a) for a in tables(tile)]
    rows = consts[0].shape[0] // 3
    kernels = spectra.shape[0]
    count = sizes[0] * sizes[1] * sizes[2]
    vmem = pl.BlockSpec(memory_space=pltpu.VMEM)
    smem = pl.BlockSpec(memory_space=pltpu.SMEM)
    dma = pltpu.SemaphoreType.DMA
    operands = tuple(
        pltpu.with_memory_space_constraint(a, pltpu.HBM) for a in (*args, *consts)
    )
    local = [
        (pltpu.SMEM if number in (9, 10) else pltpu.VMEM)(a.shape, a.dtype)
        for number, a in enumerate(operands)
    ]
    tile_shape = (tile, tile)
    error_shape = (1, 1, ITERS, site_count)
    results = pl.pallas_call(
            functools.partial(kernel, sizes),
            out_shape=(
                pltpu.VMEM(tile_shape, F32),
                pltpu.VMEM(tile_shape, F32),
                pltpu.VMEM(error_shape, F32),
                pltpu.VMEM((8, 128), F32),
            ),
            in_specs=[pl.BlockSpec(memory_space=pltpu.HBM)] * OPERANDS,
            out_specs=(vmem,) * 4,
            scratch_shapes=local
            + [
                pltpu.VMEM((2, wide, HALO), F32),
                pltpu.VMEM((4, rows, HALO), F32),
                pltpu.VMEM((2 * kernels, *spectra.shape[1:]), F32),
                pltpu.VMEM((2, 2 * tile, tile), BF16),
                pltpu.VMEM((2, 2 * tile, tile), BF16),
                pltpu.VMEM((8, BAND, BAND), F32),
                pltpu.VMEM((2, tile, tile), F32),
                pltpu.VMEM((tile, site_count), BF16),
                pltpu.VMEM((tile, tile), F32),
                pltpu.VMEM((tile, tile), F32),
                pltpu.VMEM((1, site_count), F32),
                pltpu.VMEM((1, site_count), F32),
                pltpu.VMEM((2, 128), F32),
                pltpu.VMEM((count, 2, 128), F32),
                dma((6,)),
                dma((6,)),
                dma((5,)),
                dma((5,)),
                dma((count,)),
                dma((count,)),
                pltpu.SemaphoreType.REGULAR((4,)),
                dma((OPERANDS,)),
            ],
            compiler_params=pltpu.CompilerParams(
                collective_id=0, has_side_effects=True, vmem_limit_bytes=VMEM_LIMIT
            ),
        )(*operands)
    hbm = pl.BlockSpec(memory_space=pltpu.HBM)
    return tuple(
        pl.pallas_call(
            functools.partial(write, 1.0 / (site_count * sizes[0] * sizes[1])),
            out_shape=(
                jax.ShapeDtypeStruct(tile_shape, F32),
                jax.ShapeDtypeStruct(tile_shape, F32),
                jax.ShapeDtypeStruct(error_shape, F32),
                jax.ShapeDtypeStruct((ITERS,), F32),
                jax.ShapeDtypeStruct((ITERS,), F32),
            ),
            in_specs=[vmem] * 4,
            out_specs=(hbm, hbm, hbm, smem, smem),
            scratch_shapes=[dma((3,))],
            compiler_params=pltpu.CompilerParams(vmem_limit_bytes=VMEM_LIMIT),
        )(*results)
    )


def solution(mesh):
    sizes = tuple(mesh.shape[axis] for axis in ("tx", "ty", "ka"))
    assert sizes[2] == ITERS
    placed = (
        P(("groups", "tx"), "ty"),
        P(("groups", "tx"), "ty", None),
        P(("groups", "tx"), "ty", None),
        P(("groups", "tx"), "ty", None),
        P(("groups", "tx"), "ty", None),
        P(("groups", "tx"), "ty", None, None),
        P(("groups", "tx"), "ty", None),
        P(("groups", "tx"), "ty", None),
        P("ka", None, None, None),
        P("ka"),
        P(),
    )
    return jax.shard_map(
        functools.partial(shards, sizes),
        mesh=mesh,
        in_specs=placed,
        out_specs=(
            P(("groups", "tx"), "ty"),
            P(("groups", "tx"), "ty"),
            P(("groups", "tx"), "ty", None, None),
            P("groups"),
            P("groups"),
        ),
        check_vma=False,
    )
```
